256 devices in a mesh: tm: 4 (over x), space: 64 (over z, y, core).
Axes of the slice: x: 4, y: 4, z: 8, core: 2. Of those that a mesh axis runs over, the one named last changes fastest.
Arguments:
- residual: float32 [64, 512, 8, 128], P('tm', 'space'), may hold values from -24 to 24
- capacity: float32 [512, 8, 128], P('space'), may hold values from 0.25 to 4
Outputs:
- preconditioned: float32 [64, 512, 8, 128], P('tm', 'space')
The draws below stay inside these ranges and needn't reach their ends.
All inputs are finite; a program needn't handle non-finite values.
Results may differ from the reference program's by a relative error of at most 0.0003.
Values sent between devices are 32-bit elements; how exact they have to be, the bound alone decides.
A program may use at most 64 MiB of HBM per device.

```python
import math
import jax
import jax.numpy as jnp
from jax import lax

NY = 8
NZ = 128
TSTEPS = 64
GRID_DEPTH = 4
SMOOTH = 2
COARSE_SWEEPS = 6
NX = 512


def draw_residual(key, part):
    extents = (TSTEPS, NX, NY, NZ)
    return jnp.clip(4.0 * jax.random.normal(jax.random.fold_in(key, 11), extents, jnp.float32), -24.0, 24.0)


def levels(stream_key, shape, shards, smallest, high):
    loudness = 1.0
    for dim, parts in shards:
        steps = jax.random.uniform(jax.random.fold_in(jax.random.fold_in(stream_key, 6), dim), (parts,), jnp.float32, smallest / len(shards), high / len(shards))
        loudness = loudness * jnp.repeat(jnp.exp(steps), shape[dim] // parts).reshape((-1,) + (1,) * (len(shape) - 1 - dim))
    return loudness


def setup_inputs(seed: int = 0) -> dict:
    arg_keys = jax.random.split(jax.random.key(seed), 3)
    return {
        "residual": draw_residual(jax.random.fold_in(arg_keys[2], 71), 0),
        "capacity": jnp.clip(jnp.exp(math.log(4.0) - 2.7725887 * jax.random.uniform(arg_keys[1], (NX, NY, NZ), jnp.float32) ** levels(arg_keys[1], (NX, NY, NZ), ((0, 64),), -0.2, 0.2)), 0.25, 4.0),
    }


ALPHA_CORNER = 0.01
STEP_SIZE = 0.5
DIFFUSE = 2.0
ADVECT = (0.2, -0.15, 0.1)
OMEGA = 0.7
HIGHEST = lax.Precision.HIGHEST


def level_coefficients(per_level_values):
    spread = DIFFUSE / 4.0 ** per_level_values
    drifts = tuple(component / 2.0 ** per_level_values for component in ADVECT)
    return spread, drifts


def pad_second(volume, position):
    widths = [(0, 0)] * volume.ndim
    widths[position] = (1, 1)
    return jnp.pad(volume, widths)


def apply_operator(padded, current_capacity, spectral_shifts, per_level_values):
    spread, drifts = level_coefficients(per_level_values)
    centre = padded[:, :, 1:-1]
    upper_first = padded[:, :, 2:]
    lower_first = padded[:, :, :-2]
    wide_second = pad_second(centre, 3)
    upper_second = wide_second[:, :, :, 2:]
    lower_second = wide_second[:, :, :, :-2]
    wide_third = pad_second(centre, 4)
    upper_third = wide_third[:, :, :, :, 2:]
    lower_third = wide_third[:, :, :, :, :-2]
    stencil = spread * (6.0 * centre - upper_first - lower_first - upper_second - lower_second - upper_third - lower_third)
    stencil = stencil + drifts[0] * (upper_first - lower_first) + drifts[1] * (upper_second - lower_second) + drifts[2] * (upper_third - lower_third)
    first_shift, second_shift, third_shift = spectral_shifts
    real_part = centre[0]
    imag_part = centre[1]
    shifted = jnp.stack([current_capacity * (first_shift * real_part - second_shift * imag_part), current_capacity * (second_shift * real_part + third_shift * imag_part)])
    return stencil + shifted


def inverse_diagonal(current_capacity, spectral_shifts, per_level_values):
    spread, drifts = level_coefficients(per_level_values)
    first_shift, second_shift, third_shift = spectral_shifts
    top_left = current_capacity * first_shift + 6.0 * spread
    coupling = current_capacity * second_shift
    bottom_right = current_capacity * third_shift + 6.0 * spread
    determinant = top_left * bottom_right + coupling * coupling
    return bottom_right / determinant, coupling / determinant, top_left / determinant


def damped_update(residual_now, inverse):
    diagonal_a, diagonal_b, diagonal_c = inverse
    return OMEGA * jnp.stack([diagonal_a * residual_now[0] + diagonal_b * residual_now[1], diagonal_c * residual_now[1] - diagonal_b * residual_now[0]])


def restrict_to_coarse(volume):
    leading = volume.shape[:-3]
    first_extent, second_extent, third_extent = volume.shape[-3:]
    blocks = volume.reshape(leading + (first_extent // 2, 2, second_extent // 2, 2, third_extent // 2, 2))
    lead_count = len(leading)
    return jnp.mean(blocks, axis=(lead_count + 1, lead_count + 3, lead_count + 5))


def prolong_cells(volume):
    leading = volume.shape[:-3]
    first_extent, second_extent, third_extent = volume.shape[-3:]
    expanded = jnp.broadcast_to(volume[..., :, None, :, None, :, None], leading + (first_extent, 2, second_extent, 2, third_extent, 2))
    return expanded.reshape(leading + (2 * first_extent, 2 * second_extent, 2 * third_extent))


def shift_values(frequency, length):
    ratio_step = ALPHA_CORNER ** (1.0 / length)
    phases = (2.0 * math.pi / length) * frequency.astype(jnp.float32)
    first_shift = (1.0 - ratio_step * jnp.cos(phases)) / STEP_SIZE
    second_shift = ratio_step * jnp.sin(phases) / STEP_SIZE
    return tuple(column.reshape(-1, 1, 1, 1) for column in (first_shift, second_shift, first_shift))


def multigrid_cycle(per_level_values, forcing_term, capacity_fields, spectral_shifts):
    current_capacity = capacity_fields[per_level_values]
    inverse = inverse_diagonal(current_capacity, spectral_shifts, per_level_values)
    coarsest = per_level_values == GRID_DEPTH - 1
    current = damped_update(forcing_term, inverse)
    for repeat in range((COARSE_SWEEPS if coarsest else SMOOTH) - 1):
        current = current + damped_update(forcing_term - apply_operator(pad_second(current, 2), current_capacity, spectral_shifts, per_level_values), inverse)
    if coarsest:
        return current
    coarse_right_hand = restrict_to_coarse(forcing_term - apply_operator(pad_second(current, 2), current_capacity, spectral_shifts, per_level_values))
    coarse_solution = multigrid_cycle(per_level_values + 1, coarse_right_hand, capacity_fields, spectral_shifts)
    current = current + prolong_cells(coarse_solution)
    for repeat in range(SMOOTH):
        current = current + damped_update(forcing_term - apply_operator(pad_second(current, 2), current_capacity, spectral_shifts, per_level_values), inverse)
    return current


def reference(residual, capacity):
    length = residual.shape[0]
    ratio_step = ALPHA_CORNER ** (1.0 / length)
    moments = jnp.arange(length, dtype=jnp.float32)
    weights = jnp.power(ratio_step, moments)
    scaled = residual * weights[:, None, None, None]
    capacity_fields = [capacity]
    for per_level_values in range(1, GRID_DEPTH):
        capacity_fields.append(restrict_to_coarse(capacity_fields[-1]))
    integers = jnp.arange(length, dtype=jnp.int32)

    def one_frequency(summed, frequency):
        phases = (2.0 * math.pi / length) * ((integers * frequency) % length).astype(jnp.float32)
        cosines = jnp.cos(phases)
        sines = jnp.sin(phases)
        real_part = jnp.tensordot(cosines, scaled, axes=1, precision=HIGHEST)
        imag_part = -jnp.tensordot(sines, scaled, axes=1, precision=HIGHEST)
        forcing_term = jnp.stack([real_part, imag_part])[:, None]
        spectral_shifts = shift_values(frequency[None], length)
        solution_field = multigrid_cycle(0, forcing_term, capacity_fields, spectral_shifts)[:, 0]
        summed = summed + cosines[:, None, None, None] * solution_field[0] - sines[:, None, None, None] * solution_field[1]
        return summed, None

    summed, unused = lax.scan(one_frequency, jnp.zeros(residual.shape, jnp.float32), integers)
    return summed / length / weights[:, None, None, None]
```

```python
import math

import jax
import jax.numpy as jnp
import numpy as np
from jax import lax
from jax.experimental import pallas as pl
from jax.experimental.pallas import tpu as pltpu
from jax.sharding import PartitionSpec as P

MESH = pl.DeviceIdType.MESH
F32 = jnp.float32

ALPHA_CORNER = 0.01
STEP_SIZE = 0.5
DIFFUSE = 2.0
ADVECT = (0.2, -0.15, 0.1)
OMEGA = 0.7
KEEP = 1.0 - OMEGA
LENGTH = 64
BETA = ALPHA_CORNER ** (1.0 / LENGTH)

TM = 4
SLOTS = 8
LAYERS = 8
H0 = 3
H1 = 4
REACH = 8
N0 = LAYERS + 2 * H0
N1 = LAYERS // 2 + 2 * H1
N2 = LAYERS // 4 * (1 + 2 * REACH)
N3 = N2 // 2 - 2
SHIFTS = [d for k in range(1, REACH + 1) for d in (k, -k)]

FREQUENCIES = [[0, 8, 16, 24, 4, 12, 20, 28]] + [[k + 8 * m for m in range(8)] for k in (1, 2, 3)]


def shift_tables():
    table = np.zeros((TM, 32, 8, 128), np.float64)
    for a in range(TM):
        one, two, three = [], [], []
        for slot in range(SLOTS):
            phase = 2.0 * math.pi * FREQUENCIES[a][slot] / LENGTH
            first = (1.0 - BETA * math.cos(phase)) / STEP_SIZE
            second = BETA * math.sin(phase) / STEP_SIZE
            third = first
            if a == 0 and slot == 0:
                second, third = 0.0, (1.0 + BETA) / STEP_SIZE
            one.append(first)
            two.append(second)
            three.append(third)
        for slot in range(SLOTS):
            for c, values in enumerate((one, two, three)):
                table[a, 3 * slot + c] = values[slot]
                q, sb, lb = slot // 4, slot // 2 % 2, slot % 2
                table[a, 24 + 3 * q + c, 4 * sb : 4 * sb + 4, 64 * lb : 64 * lb + 64] = values[slot]
            lanes = slice(64 * q + 32 * lb, 64 * q + 32 * lb + 32)
            table[a, 30, 2 * sb : 2 * sb + 2, lanes] = one[slot]
            table[a, 30, 4 + 2 * sb : 6 + 2 * sb, lanes] = three[slot]
            table[a, 31, 2 * sb : 2 * sb + 2, lanes] = -two[slot]
            table[a, 31, 4 + 2 * sb : 6 + 2 * sb, lanes] = two[slot]
    return table.astype(np.float32)


def plus(a, b):
    return b if a is None else a if b is None else a + b


def minus(a, b):
    return a if b is None else -b if a is None else a - b


def scaled(a, factor):
    if a is None or abs(factor) < 1e-15:
        return None
    if abs(factor - 1.0) < 1e-15:
        return a
    if abs(factor + 1.0) < 1e-15:
        return -a
    return a * np.float32(factor)


def twisted(value, phase):
    c, s = math.cos(phase), math.sin(phase)
    re, im = value
    return (minus(scaled(re, c), scaled(im, s)), plus(scaled(re, s), scaled(im, c)))


def transform(values, sign):
    n = len(values)
    if n == 1:
        return values
    even = transform(values[0::2], sign)
    odd = transform(values[1::2], sign)
    upper, lower = [], []
    for k in range(n // 2):
        turned = twisted(odd[k], sign * 2.0 * math.pi * k / n)
        upper.append((plus(even[k][0], turned[0]), plus(even[k][1], turned[1])))
        lower.append((minus(even[k][0], turned[0]), minus(even[k][1], turned[1])))
    return upper + lower


def rows_lanes():
    return (
        lax.broadcasted_iota(jnp.int32, (8, 128), 0),
        lax.broadcasted_iota(jnp.int32, (8, 128), 1),
    )


class Level:
    def __init__(self, level, ny, nz, step=1):
        row, lane = rows_lanes()
        self.spread = DIFFUSE / 4.0**level
        bx, by, bz = (b / 2.0**level for b in ADVECT)
        c = self.spread
        self.xp, self.xm = np.float32(-c + bx), np.float32(-c - bx)
        self.step = step
        self.ny = ny
        zero = jnp.zeros((8, 128), F32)
        y, z = row % 8 % max(ny, 1), lane % nz
        if ny > 1:
            self.yp = jnp.where(y < ny - 1, np.float32(-c + by), zero)
            self.ym = jnp.where(y > 0, np.float32(-c - by), zero)
        self.zp = jnp.where(z < nz - step, np.float32(-c + bz), zero)
        self.zm = jnp.where(z >= step, np.float32(-c - bz), zero)

    def neighbours(self, below, here, above):
        total = self.xp * above + self.xm * below
        total += self.zp * pltpu.roll(here, 128 - self.step, 1)
        total += self.zm * pltpu.roll(here, self.step, 1)
        if self.ny > 1:
            total += self.yp * pltpu.roll(here, 7, 0)
            total += self.ym * pltpu.roll(here, 1, 0)
        return total


def block_sum(value):
    value = value + pltpu.roll(value, 7, 0)
    return value + pltpu.roll(value, 127, 1)


def block_sum_spread(value):
    row, lane = rows_lanes()
    value = value + jnp.where(row % 2 == 0, pltpu.roll(value, 7, 0), pltpu.roll(value, 1, 0))
    return value + jnp.where(lane % 2 == 0, pltpu.roll(value, 127, 1), pltpu.roll(value, 1, 1))


def take(value, index, axis):
    return jnp.take_along_axis(value, index, axis=axis, mode="promise_in_bounds")


def pack(tiles):
    row, lane = rows_lanes()
    even_lane, even_row = lane * 2 % 128, row * 2 % 8
    halves = []
    for left, right in tiles:
        if left is right:
            halves.append(take(left, even_lane, 1))
        else:
            halves.append(jnp.where(lane < 64, take(left, even_lane, 1), take(right, even_lane, 1)))
    if tiles[0] is tiles[1]:
        return take(halves[0], even_row, 0)
    return jnp.where(row < 4, take(halves[0], even_row, 0), take(halves[1], even_row, 0))


def unpack(tile, rb, lb):
    row, lane = rows_lanes()
    return take(take(tile, 4 * rb + row // 2, 0), 64 * lb + lane // 2, 1)


def layer_of(a, l):
    return 2 * a + l + (a // 2) * (1 - 2 * l)


def kernel(
    slabs,
    res,
    cap,
    tab_in,
    out,
    tab,
    series,
    spec,
    g0,
    v0,
    c0,
    d0,
    small0,
    g1,
    v1,
    c1,
    d1,
    g2,
    w2,
    v2,
    c2,
    d2,
    d3,
    solved,
    back,
    values,
    local_sem,
    a_send,
    a_recv,
    h_send,
    h_recv,
    k_send,
    k_recv,
):
    me, my = lax.axis_index("tm"), lax.axis_index("space")

    def peer(d):
        return lax.rem(me + d, TM)

    def slab(d):
        return lax.rem(my + (d + 8 * slabs), slabs)

    barrier = pltpu.get_barrier_semaphore()
    greeted = 0
    for d in range(1, TM):
        pl.semaphore_signal(barrier, inc=1, device_id=(peer(d), my), device_id_type=MESH)
        greeted += 1
    for d in SHIFTS:
        if d % slabs:
            pl.semaphore_signal(barrier, inc=1, device_id=(me, slab(d)), device_id_type=MESH)
            greeted += 1
    pl.semaphore_wait(barrier, greeted)

    sends = []

    def remote(src, dst, send, recv, device):
        copy = pltpu.make_async_remote_copy(
            src_ref=src,
            dst_ref=dst,
            send_sem=send,
            recv_sem=recv,
            device_id=device,
            device_id_type=MESH,
        )
        copy.start()
        sends.append(copy)
        return copy

    def across(src, dst, d, send, recv):
        if d % slabs:
            copy = remote(src, dst, send, recv, (me, slab(d)))
            return copy.wait_recv
        copy = pltpu.make_async_copy(src, dst, recv)
        copy.start()
        return copy.wait

    def exchange(phase, l, source, target, own):
        waits = []
        for d in (2, 1, 3):
            n = (phase * 2 + l) * 3 + d - 1
            copy = remote(source(peer(d)), target, a_send.at[n], a_recv.at[n], (peer(d), my))
            waits.append(copy.wait_recv)
        if own is not None:
            waits.append(own())
        return waits

    def local(src, dst, n):
        copy = pltpu.make_async_copy(src, dst, local_sem.at[n])
        copy.start()
        return copy.wait

    arrive = []
    for l in range(2):
        mine = series.at[pl.ds(16 * me, 16), l]
        arrive.append(
            exchange(
                0,
                l,
                lambda j, l=l: res.at[:, layer_of(j, l)],
                mine,
                lambda l=l, mine=mine: local(res.at[:, layer_of(me, l)], mine, l),
            )
        )
    table_wait = local(tab_in.at[me], tab, 2)

    n_cap = 0
    cap_waits = []

    def spread_cap(src, dst, d):
        nonlocal n_cap
        cap_waits.append(across(src, dst, d, k_send.at[n_cap], k_recv.at[n_cap]))
        n_cap += 1

    spread_cap(cap.at[pl.ds(0, H0)], c0.at[pl.ds(H0 + LAYERS, H0)], -1)
    spread_cap(cap.at[pl.ds(LAYERS - H0, H0)], c0.at[pl.ds(0, H0)], 1)
    for i in range(LAYERS):
        c0[H0 + i] = cap[i]
    for i in range(LAYERS // 2):
        tile = block_sum(cap[2 * i] + cap[2 * i + 1]) * np.float32(0.125)
        c1[H1 + i] = pack(((tile, tile),) * 2)
    spread_cap(c1.at[pl.ds(H1, 4)], c1.at[pl.ds(H1 + 4, 4)], -1)
    spread_cap(c1.at[pl.ds(H1, 4)], c1.at[pl.ds(0, 4)], 1)
    for i in range(LAYERS // 4):
        tile = block_sum(c1[H1 + 2 * i] + c1[H1 + 2 * i + 1]) * np.float32(0.125)
        c2[2 * REACH + i] = pack(((tile, tile),) * 2)
    for d in SHIFTS:
        spread_cap(c2.at[pl.ds(2 * REACH, 2)], c2.at[pl.ds(2 * (REACH - d), 2)], d)

    table_wait()
    for wait in cap_waits:
        wait()

    def weight(index, extent):
        inside = jnp.logical_and(index >= 0, index < extent)
        return jnp.where(inside, np.float32(OMEGA), np.float32(0.0))

    six = [np.float32(6.0 * DIFFUSE / 4.0**level) for level in range(4)]

    def invert(c, first, second, third, diagonal, w):
        top, q, bottom = c * first + diagonal, c * second, c * third + diagonal
        scale = w / (top * bottom + q * q)
        return bottom * scale, q * scale, top * scale

    def invert0(slot, carry):
        first, second, third = (tab[3 * slot + k] for k in range(3))
        for i in range(N0):
            w = weight(LAYERS * my + i - H0, LAYERS * slabs)
            parts = invert(c0[i], first, second, third, six[0], w)
            for k in range(3):
                d0[slot, k, i] = parts[k]
        return carry

    lax.fori_loop(0, SLOTS, invert0, 0)
    for q in range(2):
        first, second, third = (tab[24 + 3 * q + k] for k in range(3))
        for i in range(N1):
            w = weight(4 * my + i - H1, 4 * slabs)
            parts = invert(c1[i], first, second, third, six[1], w)
            for k in range(3):
                d1[q, k, i] = parts[k]

    same, swapped = tab[30], tab[31]

    def diagonal(c, level):
        return c * same + six[level], c * swapped

    def swap(value):
        return pltpu.roll(value, 4, 0)

    def invert_packed(c, level, w):
        a, b = diagonal(c, level)
        other = swap(a)
        scale = w / (a * other + b * b)
        return other * scale, -b * scale

    for i in range(N2):
        parts = invert_packed(c2[i], 2, weight(2 * my + i - 2 * REACH, 2 * slabs))
        d2[0, i], d2[1, i] = parts
    for i in range(N3):
        c = block_sum_spread(c2[2 * i + 2] + c2[2 * i + 3]) * np.float32(0.125)
        parts = invert_packed(c, 3, weight(my + i - (REACH - 1), slabs))
        d3[0, i], d3[1, i] = parts

    def forward(l):
        middle = [[None] * 8 for _ in range(5)]
        for t2 in range(8):
            column = [
                (series[8 * t1 + t2, l] * np.float32(BETA ** (8 * t1 + t2)), None)
                for t1 in range(8)
            ]
            first = transform(column, -1.0)
            for k1 in range(5):
                middle[k1][t2] = twisted(first[k1], -2.0 * math.pi * k1 * t2 / LENGTH)
        for k1 in range(5):
            last = transform(middle[k1], -1.0)
            if k1 == 0:
                spec[0, 0, 0, l], spec[0, 1, 0, l] = last[0][0], last[4][0]
                chosen = [(m, 0, m) for m in (1, 2, 3)]
            elif k1 == 4:
                chosen = [(m, 0, 4 + m) for m in range(4)]
            else:
                chosen = [(m, k1, m) for m in range(8)]
            for m, j, slot in chosen:
                spec[j, 0, slot, l], spec[j, 1, slot, l] = last[m]

    solve = []
    for l in range(2):
        for wait in arrive[l]:
            wait()
        forward(l)
        solve.append(
            exchange(
                1,
                l,
                lambda j, l=l: spec.at[j, :, :, l],
                g0.at[:, :, H0 + layer_of(me, l)],
                None,
            )
        )
        here = H0 + layer_of(me, l)
        for c in range(2):
            for slot in range(SLOTS):
                g0[c, slot, here] = spec[me, c, slot, l]

    n_halo = 0
    halo_waits = []

    def spread_halo(src, dst, d):
        nonlocal n_halo
        halo_waits.append(across(src, dst, d, h_send.at[n_halo], h_recv.at[n_halo]))
        n_halo += 1

    for l in range(2):
        for wait in solve[l]:
            wait()
        for a in range(TM):
            x = layer_of(a, l)
            if x < H0:
                spread_halo(g0.at[:, :, H0 + x], g0.at[:, :, H0 + LAYERS + x], -1)
            if x >= LAYERS - H0:
                spread_halo(g0.at[:, :, H0 + x], g0.at[:, :, x - (LAYERS - H0)], 1)
    for wait in halo_waits:
        wait()
    halo_waits.clear()

    def jacobi(inverse, er, ei):
        a, b, c = inverse
        return a * er + b * ei, c * ei - b * er

    def sweep(level, below, here, above, g, inverse):
        er = g[0] - level.neighbours(below[0], here[0], above[0])
        ei = g[1] - level.neighbours(below[1], here[1], above[1])
        ur, ui = jacobi(inverse, er, ei)
        keep = np.float32(KEEP)
        return keep * here[0] + ur, keep * here[1] + ui

    def defect(level, below, here, above, g, c, shifts, six_here):
        first, second, third = shifts
        q = c * second
        er = g[0] - level.neighbours(below[0], here[0], above[0])
        ei = g[1] - level.neighbours(below[1], here[1], above[1])
        er = er - ((c * first + six_here) * here[0] - q * here[1])
        ei = ei - (q * here[0] + (c * third + six_here) * here[1])
        return er, ei

    def pre(level, count, own, load_g, load_d, load_c, shifts, six_here, keep_v, keep_r):
        once, twice, waiting = {}, {}, None
        for i in range(count):
            once[i] = jacobi(load_d(i), *load_g(i))
            if i < 2:
                continue
            j = i - 1
            twice[j] = sweep(level, once[j - 1], once[j], once[j + 1], load_g(j), load_d(j))
            keep_v(j, twice[j])
            j = i - 2
            if j - own[0] in range(own[1]):
                r = defect(
                    level,
                    twice[j - 1],
                    twice[j],
                    twice[j + 1],
                    load_g(j),
                    load_c(j),
                    shifts,
                    six_here,
                )
                if (j - own[0]) % 2:
                    keep_r((j - own[0]) // 2, (waiting[0] + r[0], waiting[1] + r[1]))
                waiting = r

    def post(level, first, count, load_v, load_g, load_d, keep):
        once = {}
        start = {}
        for i in range(first - 2, first + count + 2):
            start[i] = load_v(i)
            j = i - 1
            if j < first - 1:
                continue
            once[j] = sweep(level, start[j - 1], start[j], start[j + 1], load_g(j), load_d(j))
            j = i - 2
            if j < first:
                continue
            keep(j, sweep(level, once[j - 1], once[j], once[j + 1], load_g(j), load_d(j)))

    eighth = np.float32(0.125)
    level0 = Level(0, 8, 128)
    level1 = Level(1, 4, 64)
    level2 = Level(2, 2, 32)
    level3 = Level(3, 1, 32, 2)

    def down0(slot, carry):
        def keep_v(i, v):
            v0[slot, 0, i], v0[slot, 1, i] = v

        def keep_r(i, r):
            for c in range(2):
                small0[slot, c, i] = block_sum(r[c]) * eighth

        pre(
            level0,
            N0,
            (H0, LAYERS),
            lambda i: (g0[0, slot, i], g0[1, slot, i]),
            lambda i: tuple(d0[slot, k, i] for k in range(3)),
            lambda i: c0[i],
            tuple(tab[3 * slot + k] for k in range(3)),
            six[0],
            keep_v,
            keep_r,
        )
        return carry

    lax.fori_loop(0, SLOTS, down0, 0)

    for q in range(2):
        for c in range(2):
            for i in range(4):
                tiles = [[small0[4 * q + 2 * sb + lb, c, i] for lb in range(2)] for sb in range(2)]
                g1[q, c, H1 + i] = pack(tiles)
    spread_halo(g1.at[:, :, pl.ds(H1, 4)], g1.at[:, :, pl.ds(H1 + 4, 4)], -1)
    spread_halo(g1.at[:, :, pl.ds(H1, 4)], g1.at[:, :, pl.ds(0, 4)], 1)
    for wait in halo_waits:
        wait()
    halo_waits.clear()

    coarse = {}
    for q in range(2):

        def keep_v(i, v, q=q):
            v1[q, 0, i], v1[q, 1, i] = v

        def keep_r(i, r, q=q):
            for c in range(2):
                coarse[q, c, i] = block_sum(r[c]) * eighth

        pre(
            level1,
            N1,
            (H1, 4),
            lambda i, q=q: (g1[q, 0, i], g1[q, 1, i]),
            lambda i, q=q: tuple(d1[q, k, i] for k in range(3)),
            lambda i: c1[i],
            tuple(tab[24 + 3 * q + k] for k in range(3)),
            six[1],
            keep_v,
            keep_r,
        )
    for i in range(2):
        g2[2 * REACH + i] = pack([[coarse[q, c, i] for q in range(2)] for c in range(2)])
    for d in SHIFTS:
        spread_halo(g2.at[pl.ds(2 * REACH, 2)], g2.at[pl.ds(2 * (REACH - d), 2)], d)
    for wait in halo_waits:
        wait()
    halo_waits.clear()

    def relax(d, i, e):
        return d[0, i] * e + d[1, i] * swap(e)

    def sweep_packed(level, below, here, above, g, d, i):
        return np.float32(KEEP) * here + relax(d, i, g - level.neighbours(below, here, above))

    for i in range(N2):
        w2[i] = relax(d2, i, g2[i])
    for i in range(1, N2 - 1):
        v2[i] = sweep_packed(level2, w2[i - 1], w2[i], w2[i + 1], g2[i], d2, i)
    right = []
    for m in range(N3):
        pair = []
        for i in (2 * m + 2, 2 * m + 3):
            here = v2[i]
            a, b = diagonal(c2[i], 2)
            pair.append(
                g2[i]
                - level2.neighbours(v2[i - 1], here, v2[i + 1])
                - (a * here + b * swap(here))
            )
        right.append(block_sum_spread(pair[0] + pair[1]) * eighth)
    current = {m: relax(d3, m, right[m]) for m in range(N3)}
    for s in range(1, 6):
        current = {
            m: sweep_packed(
                level3, current[m - 1], current[m], current[m + 1], right[m], d3, m
            )
            for m in range(s, N3 - s)
        }
    low = 2 * 5 + 2
    stage = {i: v2[i] + current[(i - 2) // 2] for i in range(low, low + 10)}
    for s in range(1, 3):
        stage = {
            i: sweep_packed(level2, stage[i - 1], stage[i], stage[i + 1], g2[i], d2, i)
            for i in range(low + s, low + 10 - s)
        }

    for q in range(2):
        correction = {}

        def load_v(i, q=q, correction=correction):
            m = 2 * REACH + (i - H1) // 2
            if m not in correction:
                correction[m] = [unpack(stage[m], c, q) for c in range(2)]
            return tuple(v1[q, c, i] + correction[m][c] for c in range(2))

        def keep(i, v, q=q):
            v1[q, 0, i], v1[q, 1, i] = v

        post(
            level1,
            H1 - 1,
            6,
            load_v,
            lambda i, q=q: (g1[q, 0, i], g1[q, 1, i]),
            lambda i, q=q: tuple(d1[q, k, i] for k in range(3)),
            keep,
        )

    def up0(slot, carry):
        q, sb, lb = slot // 4, slot // 2 % 2, slot % 2
        correction = {}

        def load_v(i):
            m = H1 + (i - H0) // 2
            if m not in correction:
                correction[m] = [unpack(v1[q, c, m], sb, lb) for c in range(2)]
            return tuple(v0[slot, c, i] + correction[m][c] for c in range(2))

        def keep(i, v):
            solved[0, slot, i - H0], solved[1, slot, i - H0] = v

        post(
            level0,
            H0,
            LAYERS,
            load_v,
            lambda i: (g0[0, slot, i], g0[1, slot, i]),
            lambda i: tuple(d0[slot, k, i] for k in range(3)),
            keep,
        )
        return carry

    lax.fori_loop(0, SLOTS, up0, 0)

    arrive = []
    for l in range(2):
        arrive.append(
            exchange(
                2, l, lambda j, l=l: solved.at[:, :, layer_of(j, l)], back.at[me, :, :, l], None
            )
        )
        for c in range(2):
            for slot in range(SLOTS):
                back[me, c, slot, l] = solved[c, slot, layer_of(me, l)]

    def inverse(l):
        def field(j, slot, factor=2.0):
            return tuple(back[j, c, slot, l] * np.float32(factor) for c in range(2))

        nothing = (None, None)
        packed = field(0, 0, 1.0)
        line = [(packed[0], None)] + [field(0, m) for m in (1, 2, 3)] + [(packed[1], None)]
        line = transform(line + [nothing] * 3, 1.0)
        middle = [[(line[t2][0], None) for t2 in range(8)]]
        for k1 in (1, 2, 3):
            line = transform([field(k1, m) for m in range(8)], 1.0)
            middle.append(
                [twisted(line[t2], 2.0 * math.pi * k1 * t2 / LENGTH) for t2 in range(8)]
            )
        line = transform([field(0, 4 + m) for m in range(4)] + [nothing] * 4, 1.0)
        turned = [twisted(line[t2], 2.0 * math.pi * 4 * t2 / LENGTH) for t2 in range(8)]
        middle.append([(turned[t2][0], None) for t2 in range(8)])
        for t2 in range(8):
            column = transform([middle[k1][t2] for k1 in range(5)] + [nothing] * 3, 1.0)
            for t1 in range(8):
                t = 8 * t1 + t2
                values[l, t] = column[t1][0] * np.float32(BETA ** (-t) / LENGTH)

    finish = []
    for l in range(2):
        for wait in arrive[l]:
            wait()
        inverse(l)
        mine = out.at[:, layer_of(me, l)]
        finish += exchange(
            3,
            l,
            lambda j, l=l: values.at[l, pl.ds(16 * j, 16)],
            mine,
            lambda l=l, mine=mine: local(values.at[l, pl.ds(16 * me, 16)], mine, 3 + l),
        )
    for wait in finish:
        wait()
    for copy in sends:
        copy.wait_send()


def solution(mesh):
    slabs = mesh.shape["space"]
    table = shift_tables()

    def tiles(*lead):
        return pltpu.VMEM(lead + (8, 128), F32)

    def on_device(residual, capacity):
        any_space = pl.BlockSpec(memory_space=pl.ANY)
        dma = pltpu.SemaphoreType.DMA
        return pl.pallas_call(
            lambda *refs: kernel(slabs, *refs),
            out_shape=jax.ShapeDtypeStruct(residual.shape, F32),
            in_specs=[any_space, pl.BlockSpec(memory_space=pltpu.VMEM), any_space],
            out_specs=any_space,
            scratch_shapes=[
                tiles(32),
                tiles(LENGTH, 2),
                tiles(TM, 2, SLOTS, 2),
                tiles(2, SLOTS, N0),
                tiles(SLOTS, 2, N0),
                tiles(N0),
                tiles(SLOTS, 3, N0),
                tiles(SLOTS, 2, 4),
                tiles(2, 2, N1),
                tiles(2, 2, N1),
                tiles(N1),
                tiles(2, 3, N1),
                tiles(N2),
                tiles(N2),
                tiles(N2),
                tiles(N2),
                tiles(2, N2),
                tiles(2, N3),
                tiles(2, SLOTS, LAYERS),
                tiles(TM, 2, SLOTS, 2),
                tiles(2, LENGTH),
                dma((5,)),
                dma((24,)),
                dma((24,)),
                dma((24,)),
                dma((24,)),
                dma((20,)),
                dma((20,)),
            ],
            compiler_params=pltpu.CompilerParams(collective_id=0, has_side_effects=True),
            name="paradiag",
        )(residual, capacity, jnp.asarray(table))

    return jax.shard_map(
        on_device,
        mesh=mesh,
        in_specs=(P("tm", "space", None, None), P("space", None, None)),
        out_specs=P("tm", "space", None, None),
        check_vma=False,
    )
```

```python
import math

import jax
import jax.numpy as jnp
import numpy as np
from jax import lax
from jax.experimental import pallas as pl
from jax.experimental.pallas import tpu as pltpu
from jax.sharding import PartitionSpec as P

MESH = pl.DeviceIdType.MESH
F32 = jnp.float32

ALPHA_CORNER = 0.01
STEP_SIZE = 0.5
DIFFUSE = 2.0
ADVECT = (0.2, -0.15, 0.1)
OMEGA = 0.7
KEEP = 1.0 - OMEGA
LENGTH = 64
BETA = ALPHA_CORNER ** (1.0 / LENGTH)

TM = 4
SLOTS = 8
LAYERS = 8
H0 = 3
H1 = 4
REACH = 8
N0 = LAYERS + 2 * H0
N1 = LAYERS // 2 + 2 * H1
N2 = LAYERS // 4 * (1 + 2 * REACH)
N3 = N2 // 2 - 2
SHIFTS = [d for k in (4, 5, 3, 6, 2, 7, 8, 1) for d in (k, -k)]

FREQUENCIES = [[0, 8, 16, 24, 4, 12, 20, 28]] + [[k + 8 * m for m in range(8)] for k in (1, 2, 3)]


def shift_tables():
    table = np.zeros((TM, 34, 8, 128), np.float64)
    for a in range(TM):
        one, two, three = [], [], []
        for slot in range(SLOTS):
            phase = 2.0 * math.pi * FREQUENCIES[a][slot] / LENGTH
            first = (1.0 - BETA * math.cos(phase)) / STEP_SIZE
            second = BETA * math.sin(phase) / STEP_SIZE
            third = first
            if a == 0 and slot == 0:
                second, third = 0.0, (1.0 + BETA) / STEP_SIZE
            one.append(first)
            two.append(second)
            three.append(third)
        for slot in range(SLOTS):
            for c, values in enumerate((one, two, three)):
                table[a, 3 * slot + c] = values[slot]
                q, sb, lb = slot // 4, slot // 2 % 2, slot % 2
                table[a, 24 + 3 * q + c, 4 * sb : 4 * sb + 4, 64 * lb : 64 * lb + 64] = values[slot]
            for lanes in (slice(32 * lb, 32 * lb + 32), slice(64 + 32 * lb, 96 + 32 * lb)):
                table[a, 30 + 2 * q, 2 * sb : 2 * sb + 2, lanes] = one[slot]
                table[a, 30 + 2 * q, 4 + 2 * sb : 6 + 2 * sb, lanes] = three[slot]
                table[a, 31 + 2 * q, 2 * sb : 2 * sb + 2, lanes] = -two[slot]
                table[a, 31 + 2 * q, 4 + 2 * sb : 6 + 2 * sb, lanes] = two[slot]
    return table.astype(np.float32)


def plus(a, b):
    return b if a is None else a if b is None else a + b


def minus(a, b):
    return a if b is None else -b if a is None else a - b


def scaled(a, factor):
    if a is None or abs(factor) < 1e-15:
        return None
    if abs(factor - 1.0) < 1e-15:
        return a
    if abs(factor + 1.0) < 1e-15:
        return -a
    return a * np.float32(factor)


def twisted(value, phase):
    c, s = math.cos(phase), math.sin(phase)
    re, im = value
    return (minus(scaled(re, c), scaled(im, s)), plus(scaled(re, s), scaled(im, c)))


def transform(values, sign):
    n = len(values)
    if n == 1:
        return values
    even = transform(values[0::2], sign)
    odd = transform(values[1::2], sign)
    upper, lower = [], []
    for k in range(n // 2):
        turned = twisted(odd[k], sign * 2.0 * math.pi * k / n)
        upper.append((plus(even[k][0], turned[0]), plus(even[k][1], turned[1])))
        lower.append((minus(even[k][0], turned[0]), minus(even[k][1], turned[1])))
    return upper + lower


def rows_lanes():
    return (
        lax.broadcasted_iota(jnp.int32, (8, 128), 0),
        lax.broadcasted_iota(jnp.int32, (8, 128), 1),
    )


class Level:
    def __init__(self, level, ny, nz, step=1):
        row, lane = rows_lanes()
        self.spread = DIFFUSE / 4.0**level
        bx, by, bz = (b / 2.0**level for b in ADVECT)
        c = self.spread
        self.xp, self.xm = np.float32(-c + bx), np.float32(-c - bx)
        self.step = step
        self.ny = ny
        zero = jnp.zeros((8, 128), F32)
        y, z = row % 8 % max(ny, 1), lane % nz
        if ny > 1:
            self.yp = jnp.where(y < ny - 1, np.float32(-c + by), zero)
            self.ym = jnp.where(y > 0, np.float32(-c - by), zero)
        self.zp = jnp.where(z < nz - step, np.float32(-c + bz), zero)
        self.zm = jnp.where(z >= step, np.float32(-c - bz), zero)

    def neighbours(self, below, here, above):
        total = self.xp * above + self.xm * below
        total += self.zp * pltpu.roll(here, 128 - self.step, 1)
        total += self.zm * pltpu.roll(here, self.step, 1)
        if self.ny > 1:
            total += self.yp * pltpu.roll(here, 7, 0)
            total += self.ym * pltpu.roll(here, 1, 0)
        return total


def block_sum(value):
    value = value + pltpu.roll(value, 7, 0)
    return value + pltpu.roll(value, 127, 1)


def block_sum_spread(value):
    row, lane = rows_lanes()
    value = value + jnp.where(row % 2 == 0, pltpu.roll(value, 7, 0), pltpu.roll(value, 1, 0))
    return value + jnp.where(lane % 2 == 0, pltpu.roll(value, 127, 1), pltpu.roll(value, 1, 1))


def take(value, index, axis):
    return jnp.take_along_axis(value, index, axis=axis, mode="promise_in_bounds")


def pack(tiles):
    row, lane = rows_lanes()
    even_lane, even_row = lane * 2 % 128, row * 2 % 8
    halves = []
    for left, right in tiles:
        if left is right:
            halves.append(take(left, even_lane, 1))
        else:
            halves.append(jnp.where(lane < 64, take(left, even_lane, 1), take(right, even_lane, 1)))
    if tiles[0] is tiles[1]:
        return take(halves[0], even_row, 0)
    return jnp.where(row < 4, take(halves[0], even_row, 0), take(halves[1], even_row, 0))


def unpack(tile, rb, lb):
    row, lane = rows_lanes()
    return take(take(tile, 4 * rb + row // 2, 0), 64 * lb + lane // 2, 1)


def layer_of(a, l):
    return 2 * a + l + (a // 2) * (1 - 2 * l)


def kernel(
    slabs,
    res_in,
    cap_in,
    tab_in,
    out,
    res,
    cap,
    tab,
    series,
    spec,
    g0,
    v0,
    c0,
    d0,
    small0,
    g1,
    v1,
    c1,
    d1,
    g2,
    w2,
    v2,
    c2,
    d2,
    d3,
    solved,
    back,
    values,
    local_sem,
    a_send,
    a_recv,
    h_send,
    h_recv,
    k_send,
    k_recv,
):
    me, my = lax.axis_index("tm"), lax.axis_index("space")

    def peer(d):
        return lax.rem(me + d, TM)

    def slab(d):
        return lax.rem(my + (d + 8 * slabs), slabs)

    def local(src, dst, n):
        copy = pltpu.make_async_copy(src, dst, local_sem.at[n])
        copy.start()
        return copy.wait

    res_wait = local(res_in, res, 0)
    cap_wait = local(cap_in, cap, 1)
    table_wait = local(tab_in.at[me], tab, 2)

    barrier = pltpu.get_barrier_semaphore()
    greeted = 0
    for d in range(1, TM):
        pl.semaphore_signal(barrier, inc=1, device_id=(peer(d), my), device_id_type=MESH)
        greeted += 1
    for d in SHIFTS:
        if d % slabs:
            pl.semaphore_signal(barrier, inc=1, device_id=(me, slab(d)), device_id_type=MESH)
            greeted += 1
    pl.semaphore_wait(barrier, greeted)

    sends = []

    def remote(src, dst, send, recv, device):
        copy = pltpu.make_async_remote_copy(
            src_ref=src,
            dst_ref=dst,
            send_sem=send,
            recv_sem=recv,
            device_id=device,
            device_id_type=MESH,
        )
        copy.start()
        sends.append(copy)
        return copy

    def across(src, dst, d, send, recv):
        if d % slabs:
            copy = remote(src, dst, send, recv, (me, slab(d)))
            return copy.wait_recv
        copy = pltpu.make_async_copy(src, dst, recv)
        copy.start()
        return copy.wait

    def exchange(first, source, target):
        waits = []
        for d in (2, 1, 3):
            n = first + d - 1
            copy = remote(source(peer(d)), target, a_send.at[n], a_recv.at[n], (peer(d), my))
            waits.append(copy.wait_recv)
        return waits

    res_wait()
    arrive = []
    for l in range(2):
        arrive.append(
            exchange(
                3 * l,
                lambda j, l=l: res.at[:, layer_of(j, l)],
                series.at[pl.ds(16 * me, 16), l],
            )
        )
    for l in range(2):
        for t in range(16):
            series[16 * me + t, l] = res[t, layer_of(me, l)]

    cap_wait()
    n_cap = 0
    cap_waits = []

    def spread_cap(src, dst, d):
        nonlocal n_cap
        cap_waits.append(across(src, dst, d, k_send.at[n_cap], k_recv.at[n_cap]))
        n_cap += 1

    spread_cap(cap.at[pl.ds(0, H0)], c0.at[pl.ds(H0 + LAYERS, H0)], -1)
    spread_cap(cap.at[pl.ds(LAYERS - H0, H0)], c0.at[pl.ds(0, H0)], 1)
    for i in range(LAYERS):
        c0[H0 + i] = cap[i]
    for i in range(LAYERS // 2):
        tile = block_sum(cap[2 * i] + cap[2 * i + 1]) * np.float32(0.125)
        c1[H1 + i] = pack(((tile, tile),) * 2)
    spread_cap(c1.at[pl.ds(H1, 4)], c1.at[pl.ds(H1 + 4, 4)], -1)
    spread_cap(c1.at[pl.ds(H1, 4)], c1.at[pl.ds(0, 4)], 1)
    for i in range(LAYERS // 4):
        tile = block_sum(c1[H1 + 2 * i] + c1[H1 + 2 * i + 1]) * np.float32(0.125)
        c2[2 * REACH + i] = pack(((tile, tile),) * 2)
    for d in SHIFTS:
        spread_cap(c2.at[pl.ds(2 * REACH, 2)], c2.at[pl.ds(2 * (REACH - d), 2)], d)

    def forward(l):
        middle = [[None] * 8 for _ in range(5)]
        for t2 in range(8):
            column = [
                (series[8 * t1 + t2, l] * np.float32(BETA ** (8 * t1 + t2)), None)
                for t1 in range(8)
            ]
            first = transform(column, -1.0)
            for k1 in range(5):
                middle[k1][t2] = twisted(first[k1], -2.0 * math.pi * k1 * t2 / LENGTH)
        for k1 in range(5):
            last = transform(middle[k1], -1.0)
            if k1 == 0:
                spec[0, 0, 0, l], spec[0, 1, 0, l] = last[0][0], last[4][0]
                chosen = [(m, 0, m) for m in (1, 2, 3)]
            elif k1 == 4:
                chosen = [(m, 0, 4 + m) for m in range(4)]
            else:
                chosen = [(m, k1, m) for m in range(8)]
            for m, j, slot in chosen:
                spec[j, 0, slot, l], spec[j, 1, slot, l] = last[m]

    solve = {}
    for l in range(2):
        for wait in arrive[l]:
            wait()
        forward(l)
        for q in range(2):
            four = pl.ds(4 * q, 4)
            solve[l, q] = exchange(
                6 + 6 * l + 3 * q,
                lambda j, l=l, four=four: spec.at[j, :, four, l],
                g0.at[:, four, H0 + layer_of(me, l)],
            )
        here = H0 + layer_of(me, l)
        for c in range(2):
            for slot in range(SLOTS):
                g0[c, slot, here] = spec[me, c, slot, l]

    table_wait()
    for wait in cap_waits:
        wait()

    def weight(index, extent):
        inside = jnp.logical_and(index >= 0, index < extent)
        return jnp.where(inside, np.float32(OMEGA), np.float32(0.0))

    six = [np.float32(6.0 * DIFFUSE / 4.0**level) for level in range(4)]

    def invert(c, first, second, third, diagonal, w):
        top, q, bottom = c * first + diagonal, c * second, c * third + diagonal
        scale = w / (top * bottom + q * q)
        return bottom * scale, q * scale, top * scale

    def invert0(slot, carry):
        first, second, third = (tab[3 * slot + k] for k in range(3))
        for i in range(N0):
            w = weight(LAYERS * my + i - H0, LAYERS * slabs)
            parts = invert(c0[i], first, second, third, six[0], w)
            for k in range(3):
                d0[slot, k, i] = parts[k]
        return carry

    lax.fori_loop(0, SLOTS, invert0, 0)
    for q in range(2):
        first, second, third = (tab[24 + 3 * q + k] for k in range(3))
        for i in range(N1):
            w = weight(4 * my + i - H1, 4 * slabs)
            parts = invert(c1[i], first, second, third, six[1], w)
            for k in range(3):
                d1[q, k, i] = parts[k]

    def diagonal(c, q, level):
        return c * tab[30 + 2 * q] + six[level], c * tab[31 + 2 * q]

    def swap(value):
        return pltpu.roll(value, 4, 0)

    def invert_packed(c, q, level, w):
        a, b = diagonal(c, q, level)
        other = swap(a)
        scale = w / (a * other + b * b)
        return other * scale, -b * scale

    for i in range(N2):
        w = weight(2 * my + i - 2 * REACH, 2 * slabs)
        for q in range(2):
            parts = invert_packed(c2[i], q, 2, w)
            d2[q, 0, i], d2[q, 1, i] = parts
    for i in range(N3):
        c = block_sum_spread(c2[2 * i + 2] + c2[2 * i + 3]) * np.float32(0.125)
        w = weight(my + i - (REACH - 1), slabs)
        for q in range(2):
            parts = invert_packed(c, q, 3, w)
            d3[q, 0, i], d3[q, 1, i] = parts

    n_halo = 0

    def spread(src, dst, d):
        nonlocal n_halo
        n_halo += 1
        return across(src, dst, d, h_send.at[n_halo - 1], h_recv.at[n_halo - 1])

    halo = {0: [], 1: []}
    for l in range(2):
        for q in range(2):
            for wait in solve[l, q]:
                wait()
            four = pl.ds(4 * q, 4)
            for a in range(TM):
                x = layer_of(a, l)
                here = g0.at[:, four, H0 + x]
                if x < H0:
                    halo[q].append(spread(here, g0.at[:, four, H0 + LAYERS + x], -1))
                if x >= LAYERS - H0:
                    halo[q].append(spread(here, g0.at[:, four, x - (LAYERS - H0)], 1))

    def jacobi(inverse, er, ei):
        a, b, c = inverse
        return a * er + b * ei, c * ei - b * er

    def sweep(level, below, here, above, g, inverse):
        er = g[0] - level.neighbours(below[0], here[0], above[0])
        ei = g[1] - level.neighbours(below[1], here[1], above[1])
        ur, ui = jacobi(inverse, er, ei)
        keep = np.float32(KEEP)
        return keep * here[0] + ur, keep * here[1] + ui

    def defect(level, below, here, above, g, c, shifts, six_here):
        first, second, third = shifts
        q = c * second
        er = g[0] - level.neighbours(below[0], here[0], above[0])
        ei = g[1] - level.neighbours(below[1], here[1], above[1])
        er = er - ((c * first + six_here) * here[0] - q * here[1])
        ei = ei - (q * here[0] + (c * third + six_here) * here[1])
        return er, ei

    def pre(level, count, own, load_g, load_d, load_c, shifts, six_here, keep_v, keep_r):
        once, twice, waiting = {}, {}, None
        for i in range(count):
            once[i] = jacobi(load_d(i), *load_g(i))
            if i < 2:
                continue
            j = i - 1
            twice[j] = sweep(level, once[j - 1], once[j], once[j + 1], load_g(j), load_d(j))
            keep_v(j, twice[j])
            j = i - 2
            if j - own[0] in range(own[1]):
                r = defect(
                    level,
                    twice[j - 1],
                    twice[j],
                    twice[j + 1],
                    load_g(j),
                    load_c(j),
                    shifts,
                    six_here,
                )
                if (j - own[0]) % 2:
                    keep_r((j - own[0]) // 2, (waiting[0] + r[0], waiting[1] + r[1]))
                waiting = r

    def post(level, first, count, load_v, load_g, load_d, keep):
        once = {}
        start = {}
        for i in range(first - 2, first + count + 2):
            start[i] = load_v(i)
            j = i - 1
            if j < first - 1:
                continue
            once[j] = sweep(level, start[j - 1], start[j], start[j + 1], load_g(j), load_d(j))
            j = i - 2
            if j < first:
                continue
            keep(j, sweep(level, once[j - 1], once[j], once[j + 1], load_g(j), load_d(j)))

    eighth = np.float32(0.125)
    level0 = Level(0, 8, 128)
    level1 = Level(1, 4, 64)
    level2 = Level(2, 2, 32)
    level3 = Level(3, 1, 32, 2)

    def down0(slot, carry):
        def keep_v(i, v):
            v0[slot, 0, i], v0[slot, 1, i] = v

        def keep_r(i, r):
            for c in range(2):
                small0[slot, c, i] = block_sum(r[c]) * eighth

        pre(
            level0,
            N0,
            (H0, LAYERS),
            lambda i: (g0[0, slot, i], g0[1, slot, i]),
            lambda i: tuple(d0[slot, k, i] for k in range(3)),
            lambda i: c0[i],
            tuple(tab[3 * slot + k] for k in range(3)),
            six[0],
            keep_v,
            keep_r,
        )
        return carry

    for q in range(2):
        for wait in halo[q]:
            wait()
        lax.fori_loop(4 * q, 4 * q + 4, down0, 0)
        for c in range(2):
            for i in range(4):
                tiles = [[small0[4 * q + 2 * sb + lb, c, i] for lb in range(2)] for sb in range(2)]
                g1[q, c, H1 + i] = pack(tiles)
        mine = g1.at[q, :, pl.ds(H1, 4)]
        halo[q] = [
            spread(mine, g1.at[q, :, pl.ds(H1 + 4, 4)], -1),
            spread(mine, g1.at[q, :, pl.ds(0, 4)], 1),
        ]

    for q in range(2):
        for wait in halo[q]:
            wait()
        coarse = {}

        def keep_v(i, v, q=q):
            v1[q, 0, i], v1[q, 1, i] = v

        def keep_r(i, r, coarse=coarse):
            for c in range(2):
                coarse[c, i] = block_sum(r[c]) * eighth

        pre(
            level1,
            N1,
            (H1, 4),
            lambda i, q=q: (g1[q, 0, i], g1[q, 1, i]),
            lambda i, q=q: tuple(d1[q, k, i] for k in range(3)),
            lambda i: c1[i],
            tuple(tab[24 + 3 * q + k] for k in range(3)),
            six[1],
            keep_v,
            keep_r,
        )
        for i in range(2):
            g2[q, 2 * REACH + i] = pack([[coarse[c, i], coarse[c, i]] for c in range(2)])
        halo[q] = [
            spread(g2.at[q, pl.ds(2 * REACH, 2)], g2.at[q, pl.ds(2 * (REACH - d), 2)], d)
            for d in SHIFTS
        ]

    def relax(d, q, i, e):
        return d[q, 0, i] * e + d[q, 1, i] * swap(e)

    def sweep_packed(level, below, here, above, g, d, q, i):
        return np.float32(KEEP) * here + relax(d, q, i, g - level.neighbours(below, here, above))

    def coarse_levels(q):
        for i in range(N2):
            w2[i] = relax(d2, q, i, g2[q, i])
        for i in range(1, N2 - 1):
            v2[i] = sweep_packed(level2, w2[i - 1], w2[i], w2[i + 1], g2[q, i], d2, q, i)
        right = []
        for m in range(N3):
            pair = []
            for i in (2 * m + 2, 2 * m + 3):
                here = v2[i]
                a, b = diagonal(c2[i], q, 2)
                pair.append(
                    g2[q, i]
                    - level2.neighbours(v2[i - 1], here, v2[i + 1])
                    - (a * here + b * swap(here))
                )
            right.append(block_sum_spread(pair[0] + pair[1]) * eighth)
        current = {m: relax(d3, q, m, right[m]) for m in range(N3)}
        for s in range(1, 6):
            current = {
                m: sweep_packed(
                    level3, current[m - 1], current[m], current[m + 1], right[m], d3, q, m
                )
                for m in range(s, N3 - s)
            }
        low = 2 * 5 + 2
        stage = {i: v2[i] + current[(i - 2) // 2] for i in range(low, low + 10)}
        for s in range(1, 3):
            stage = {
                i: sweep_packed(level2, stage[i - 1], stage[i], stage[i + 1], g2[q, i], d2, q, i)
                for i in range(low + s, low + 10 - s)
            }
        return stage

    def up1(q, stage):
        correction = {}

        def load_v(i):
            m = 2 * REACH + (i - H1) // 2
            if m not in correction:
                correction[m] = [unpack(stage[m], c, 0) for c in range(2)]
            return tuple(v1[q, c, i] + correction[m][c] for c in range(2))

        def keep(i, v):
            v1[q, 0, i], v1[q, 1, i] = v

        post(
            level1,
            H1 - 1,
            6,
            load_v,
            lambda i: (g1[q, 0, i], g1[q, 1, i]),
            lambda i: tuple(d1[q, k, i] for k in range(3)),
            keep,
        )

    def up0(slot, carry):
        q, sb, lb = slot // 4, slot // 2 % 2, slot % 2
        correction = {}

        def load_v(i):
            m = H1 + (i - H0) // 2
            if m not in correction:
                correction[m] = [unpack(v1[q, c, m], sb, lb) for c in range(2)]
            return tuple(v0[slot, c, i] + correction[m][c] for c in range(2))

        def keep(i, v):
            solved[0, slot, i - H0], solved[1, slot, i - H0] = v

        post(
            level0,
            H0,
            LAYERS,
            load_v,
            lambda i: (g0[0, slot, i], g0[1, slot, i]),
            lambda i: tuple(d0[slot, k, i] for k in range(3)),
            keep,
        )
        return carry

    arrive = [[], []]
    for q in range(2):
        for wait in halo[q]:
            wait()
        stage = coarse_levels(q)
        up1(q, stage)
        lax.fori_loop(4 * q, 4 * q + 4, up0, 0)
        four = pl.ds(4 * q, 4)
        for l in range(2):
            arrive[l] += exchange(
                18 + 6 * q + 3 * l,
                lambda j, l=l, four=four: solved.at[:, four, layer_of(j, l)],
                back.at[me, :, four, l],
            )
        for l in range(2):
            for c in range(2):
                for slot in range(4 * q, 4 * q + 4):
                    back[me, c, slot, l] = solved[c, slot, layer_of(me, l)]

    def inverse(l):
        def field(j, slot, factor=2.0):
            return tuple(back[j, c, slot, l] * np.float32(factor) for c in range(2))

        nothing = (None, None)
        packed = field(0, 0, 1.0)
        line = [(packed[0], None)] + [field(0, m) for m in (1, 2, 3)] + [(packed[1], None)]
        line = transform(line + [nothing] * 3, 1.0)
        middle = [[(line[t2][0], None) for t2 in range(8)]]
        for k1 in (1, 2, 3):
            line = transform([field(k1, m) for m in range(8)], 1.0)
            middle.append(
                [twisted(line[t2], 2.0 * math.pi * k1 * t2 / LENGTH) for t2 in range(8)]
            )
        line = transform([field(0, 4 + m) for m in range(4)] + [nothing] * 4, 1.0)
        turned = [twisted(line[t2], 2.0 * math.pi * 4 * t2 / LENGTH) for t2 in range(8)]
        middle.append([(turned[t2][0], None) for t2 in range(8)])
        for t2 in range(8):
            column = transform([middle[k1][t2] for k1 in range(5)] + [nothing] * 3, 1.0)
            for t1 in range(8):
                t = 8 * t1 + t2
                values[l, t] = column[t1][0] * np.float32(BETA ** (-t) / LENGTH)

    finish = []
    for l in range(2):
        for wait in arrive[l]:
            wait()
        inverse(l)
        mine = out.at[:, layer_of(me, l)]
        finish += exchange(30 + 3 * l, lambda j, l=l: values.at[l, pl.ds(16 * j, 16)], mine)
        finish.append(local(values.at[l, pl.ds(16 * me, 16)], mine, 3 + l))
    for wait in finish:
        wait()
    for copy in sends:
        copy.wait_send()


def solution(mesh):
    slabs = mesh.shape["space"]
    table = shift_tables()

    def tiles(*lead):
        return pltpu.VMEM(lead + (8, 128), F32)

    def on_device(residual, capacity):
        any_space = pl.BlockSpec(memory_space=pl.ANY)
        dma = pltpu.SemaphoreType.DMA
        return pl.pallas_call(
            lambda *refs: kernel(slabs, *refs),
            out_shape=jax.ShapeDtypeStruct(residual.shape, F32),
            in_specs=[any_space] * 3,
            out_specs=any_space,
            scratch_shapes=[
                tiles(16, LAYERS),
                tiles(LAYERS),
                tiles(34),
                tiles(LENGTH, 2),
                tiles(TM, 2, SLOTS, 2),
                tiles(2, SLOTS, N0),
                tiles(SLOTS, 2, N0),
                tiles(N0),
                tiles(SLOTS, 3, N0),
                tiles(SLOTS, 2, 4),
                tiles(2, 2, N1),
                tiles(2, 2, N1),
                tiles(N1),
                tiles(2, 3, N1),
                tiles(2, N2),
                tiles(N2),
                tiles(N2),
                tiles(N2),
                tiles(2, 2, N2),
                tiles(2, 2, N3),
                tiles(2, SLOTS, LAYERS),
                tiles(TM, 2, SLOTS, 2),
                tiles(2, LENGTH),
                dma((5,)),
                dma((36,)),
                dma((36,)),
                dma((48,)),
                dma((48,)),
                dma((20,)),
                dma((20,)),
            ],
            compiler_params=pltpu.CompilerParams(collective_id=0, has_side_effects=True),
            name="paradiag",
        )(residual, capacity, jnp.asarray(table))

    return jax.shard_map(
        on_device,
        mesh=mesh,
        in_specs=(P("tm", "space", None, None), P("space", None, None)),
        out_specs=P("tm", "space", None, None),
        check_vma=False,
    )
```

```python
import math

import jax
import jax.numpy as jnp
import numpy as np
from jax import lax
from jax.experimental import pallas as pl
from jax.experimental.pallas import tpu as pltpu
from jax.sharding import PartitionSpec as P

MESH = pl.DeviceIdType.MESH
F32 = jnp.float32

ALPHA_CORNER = 0.01
STEP_SIZE = 0.5
DIFFUSE = 2.0
ADVECT = (0.2, -0.15, 0.1)
OMEGA = 0.7
KEEP = 1.0 - OMEGA
LENGTH = 64
BETA = ALPHA_CORNER ** (1.0 / LENGTH)

TM = 4
SLOTS = 8
LAYERS = 8
H0 = 3
H1 = 4
REACH = 8
N0 = LAYERS + 2 * H0
N1 = LAYERS // 2 + 2 * H1
N2 = LAYERS // 4 * (1 + 2 * REACH)
N3 = N2 // 2 - 2
SHIFTS = [d for k in (4, 5, 3, 6, 2, 7, 8, 1) for d in (k, -k)]

FREQUENCIES = [[0, 8, 16, 24, 4, 12, 20, 28]] + [[k + 8 * m for m in range(8)] for k in (1, 2, 3)]


def shift_tables():
    table = np.zeros((TM, 34, 8, 128), np.float64)
    for a in range(TM):
        one, two, three = [], [], []
        for slot in range(SLOTS):
            phase = 2.0 * math.pi * FREQUENCIES[a][slot] / LENGTH
            first = (1.0 - BETA * math.cos(phase)) / STEP_SIZE
            second = BETA * math.sin(phase) / STEP_SIZE
            third = first
            if a == 0 and slot == 0:
                second, third = 0.0, (1.0 + BETA) / STEP_SIZE
            one.append(first)
            two.append(second)
            three.append(third)
        for slot in range(SLOTS):
            for c, values in enumerate((one, two, three)):
                table[a, 3 * slot + c] = values[slot]
                q, sb, lb = slot // 4, slot // 2 % 2, slot % 2
                table[a, 24 + 3 * q + c, 4 * sb : 4 * sb + 4, 64 * lb : 64 * lb + 64] = values[slot]
            for lanes in (slice(32 * lb, 32 * lb + 32), slice(64 + 32 * lb, 96 + 32 * lb)):
                table[a, 30 + 2 * q, 2 * sb : 2 * sb + 2, lanes] = one[slot]
                table[a, 30 + 2 * q, 4 + 2 * sb : 6 + 2 * sb, lanes] = three[slot]
                table[a, 31 + 2 * q, 2 * sb : 2 * sb + 2, lanes] = -two[slot]
                table[a, 31 + 2 * q, 4 + 2 * sb : 6 + 2 * sb, lanes] = two[slot]
    return table.astype(np.float32)


def plus(a, b):
    return b if a is None else a if b is None else a + b


def minus(a, b):
    return a if b is None else -b if a is None else a - b


def scaled(a, factor):
    if a is None or abs(factor) < 1e-15:
        return None
    if abs(factor - 1.0) < 1e-15:
        return a
    if abs(factor + 1.0) < 1e-15:
        return -a
    return a * np.float32(factor)


def twisted(value, phase):
    c, s = math.cos(phase), math.sin(phase)
    re, im = value
    return (minus(scaled(re, c), scaled(im, s)), plus(scaled(re, s), scaled(im, c)))


def transform(values, sign):
    n = len(values)
    if n == 1:
        return values
    even = transform(values[0::2], sign)
    odd = transform(values[1::2], sign)
    upper, lower = [], []
    for k in range(n // 2):
        turned = twisted(odd[k], sign * 2.0 * math.pi * k / n)
        upper.append((plus(even[k][0], turned[0]), plus(even[k][1], turned[1])))
        lower.append((minus(even[k][0], turned[0]), minus(even[k][1], turned[1])))
    return upper + lower


def rows_lanes():
    return (
        lax.broadcasted_iota(jnp.int32, (8, 128), 0),
        lax.broadcasted_iota(jnp.int32, (8, 128), 1),
    )


class Level:
    def __init__(self, level, ny, nz, step=1):
        row, lane = rows_lanes()
        self.spread = DIFFUSE / 4.0**level
        bx, by, bz = (b / 2.0**level for b in ADVECT)
        c = self.spread
        self.xp, self.xm = np.float32(-c + bx), np.float32(-c - bx)
        self.step = step
        self.ny = ny
        zero = jnp.zeros((8, 128), F32)
        y, z = row % 8 % max(ny, 1), lane % nz
        if ny > 1:
            self.yp = jnp.where(y < ny - 1, np.float32(-c + by), zero)
            self.ym = jnp.where(y > 0, np.float32(-c - by), zero)
        self.zp = jnp.where(z < nz - step, np.float32(-c + bz), zero)
        self.zm = jnp.where(z >= step, np.float32(-c - bz), zero)

    def neighbours(self, below, here, above):
        total = self.xp * above + self.xm * below
        total += self.zp * pltpu.roll(here, 128 - self.step, 1)
        total += self.zm * pltpu.roll(here, self.step, 1)
        if self.ny > 1:
            total += self.yp * pltpu.roll(here, 7, 0)
            total += self.ym * pltpu.roll(here, 1, 0)
        return total


def block_sum(value):
    value = value + pltpu.roll(value, 7, 0)
    return value + pltpu.roll(value, 127, 1)


def block_sum_spread(value):
    row, lane = rows_lanes()
    value = value + jnp.where(row % 2 == 0, pltpu.roll(value, 7, 0), pltpu.roll(value, 1, 0))
    return value + jnp.where(lane % 2 == 0, pltpu.roll(value, 127, 1), pltpu.roll(value, 1, 1))


def take(value, index, axis):
    return jnp.take_along_axis(value, index, axis=axis, mode="promise_in_bounds")


def pack(tiles):
    row, lane = rows_lanes()
    even_lane, even_row = lane * 2 % 128, row * 2 % 8
    halves = []
    for left, right in tiles:
        if left is right:
            halves.append(take(left, even_lane, 1))
        else:
            halves.append(jnp.where(lane < 64, take(left, even_lane, 1), take(right, even_lane, 1)))
    if tiles[0] is tiles[1]:
        return take(halves[0], even_row, 0)
    return jnp.where(row < 4, take(halves[0], even_row, 0), take(halves[1], even_row, 0))


def unpack(tile, rb, lb):
    row, lane = rows_lanes()
    return take(take(tile, 4 * rb + row // 2, 0), 64 * lb + lane // 2, 1)


def layer_of(a, l):
    return 2 * a + l + (a // 2) * (1 - 2 * l)


def kernel(
    slabs,
    res_in,
    cap_in,
    tab_in,
    out,
    res,
    cap,
    tab,
    series,
    spec,
    g0,
    v0,
    c0,
    d0,
    small0,
    g1,
    v1,
    c1,
    d1,
    g2,
    w2,
    v2,
    c2,
    d2,
    d3,
    solved,
    back,
    values,
    p2,
    local_sem,
    send_sem,
    recv_sem,
):
    me, my = lax.axis_index("tm"), lax.axis_index("space")

    def peer(d):
        return lax.rem(me + d, TM)

    def slab(d):
        return lax.rem(my + (d + 8 * slabs), slabs)

    def local(src, dst, n):
        copy = pltpu.make_async_copy(src, dst, local_sem.at[n])
        copy.start()
        return copy.wait

    res_wait = local(res_in, res, 0)
    cap_wait = local(cap_in, cap, 1)
    table_wait = local(tab_in.at[me], tab, 2)

    barrier = pltpu.get_barrier_semaphore()
    greeted = 0
    for d in range(1, TM):
        pl.semaphore_signal(barrier, inc=1, device_id=(peer(d), my), device_id_type=MESH)
        greeted += 1
    for d in SHIFTS:
        if d % slabs:
            pl.semaphore_signal(barrier, inc=1, device_id=(me, slab(d)), device_id_type=MESH)
            greeted += 1
    pl.semaphore_wait(barrier, greeted)

    def remote(src, dst, out_sem, in_sem, device):
        pltpu.make_async_remote_copy(
            src_ref=src,
            dst_ref=dst,
            send_sem=send_sem.at[out_sem],
            recv_sem=recv_sem.at[in_sem],
            device_id=device,
            device_id_type=MESH,
        ).start()

    def landed(size, n):
        pltpu.make_async_copy(size, size, recv_sem.at[n]).wait()

    def sent(size, n):
        pltpu.make_async_copy(size, size, send_sem.at[n]).wait()

    def exchange(out_sem, in_sem, source, target):
        for d in (2, 1, 3):
            remote(source(peer(d)), target, out_sem, in_sem, (peer(d), my))

    res_wait()
    for l in range(2):
        exchange(
            0,
            0 + l,
            lambda j, l=l: res.at[:, layer_of(j, l)],
            series.at[pl.ds(16 * me, 16), l],
        )
    for l in range(2):
        for t in range(16):
            series[16 * me + t, l] = res[t, layer_of(me, l)]

    cap_wait()

    def spread_cap(src, dst, d):
        remote(src, dst, 7, 15, (me, slab(d)))

    spread_cap(cap.at[pl.ds(0, H0)], c0.at[pl.ds(H0 + LAYERS, H0)], -1)
    spread_cap(cap.at[pl.ds(LAYERS - H0, H0)], c0.at[pl.ds(0, H0)], 1)
    for i in range(LAYERS):
        c0[H0 + i] = cap[i]
    for i in range(LAYERS // 2):
        tile = block_sum(cap[2 * i] + cap[2 * i + 1]) * np.float32(0.125)
        c1[H1 + i] = pack(((tile, tile),) * 2)
    spread_cap(c1.at[pl.ds(H1, 4)], c1.at[pl.ds(H1 + 4, 4)], -1)
    spread_cap(c1.at[pl.ds(H1, 4)], c1.at[pl.ds(0, 4)], 1)
    for i in range(LAYERS // 4):
        tile = block_sum(c1[H1 + 2 * i] + c1[H1 + 2 * i + 1]) * np.float32(0.125)
        c2[2 * REACH + i] = pack(((tile, tile),) * 2)
    for d in SHIFTS:
        spread_cap(c2.at[pl.ds(2 * REACH, 2)], c2.at[pl.ds(2 * (REACH - d), 2)], d)

    def forward(l):
        middle = [[None] * 8 for _ in range(5)]
        for t2 in range(8):
            column = [
                (series[8 * t1 + t2, l] * np.float32(BETA ** (8 * t1 + t2)), None)
                for t1 in range(8)
            ]
            first = transform(column, -1.0)
            for k1 in range(5):
                middle[k1][t2] = twisted(first[k1], -2.0 * math.pi * k1 * t2 / LENGTH)
        for k1 in range(5):
            last = transform(middle[k1], -1.0)
            if k1 == 0:
                spec[0, 0, 0, l], spec[0, 1, 0, l] = last[0][0], last[4][0]
                chosen = [(m, 0, m) for m in (1, 2, 3)]
            elif k1 == 4:
                chosen = [(m, 0, 4 + m) for m in range(4)]
            else:
                chosen = [(m, k1, m) for m in range(8)]
            for m, j, slot in chosen:
                spec[j, 0, slot, l], spec[j, 1, slot, l] = last[m]

    for l in range(2):
        landed(series.at[pl.ds(0, 48), l], l)
        forward(l)
        for q in range(2):
            four = pl.ds(4 * q, 4)
            exchange(
                1,
                2 + 2 * l + q,
                lambda j, l=l, four=four: spec.at[j, :, four, l],
                g0.at[:, four, H0 + layer_of(me, l)],
            )
        here = H0 + layer_of(me, l)
        for c in range(2):
            for slot in range(SLOTS):
                g0[c, slot, here] = spec[me, c, slot, l]

    table_wait()
    landed(series.at[pl.ds(0, 46), 0], 15)

    def weight(index, extent):
        inside = jnp.logical_and(index >= 0, index < extent)
        return jnp.where(inside, np.float32(OMEGA), np.float32(0.0))

    six = [np.float32(6.0 * DIFFUSE / 4.0**level) for level in range(4)]

    def invert(c, first, second, third, diagonal, w):
        top, q, bottom = c * first + diagonal, c * second, c * third + diagonal
        scale = w / (top * bottom + q * q)
        return bottom * scale, q * scale, top * scale

    def invert0(slot, carry):
        first, second, third = (tab[3 * slot + k] for k in range(3))
        for i in range(N0):
            w = weight(LAYERS * my + i - H0, LAYERS * slabs)
            parts = invert(c0[i], first, second, third, six[0], w)
            for k in range(3):
                d0[slot, k, i] = parts[k]
        return carry

    lax.fori_loop(0, SLOTS, invert0, 0)
    for q in range(2):
        first, second, third = (tab[24 + 3 * q + k] for k in range(3))
        for i in range(N1):
            w = weight(4 * my + i - H1, 4 * slabs)
            parts = invert(c1[i], first, second, third, six[1], w)
            for k in range(3):
                d1[q, k, i] = parts[k]

    def diagonal(c, q, level):
        return c * tab[30 + 2 * q] + six[level], c * tab[31 + 2 * q]

    def swap(value):
        return pltpu.roll(value, 4, 0)

    def invert_packed(c, q, level, w):
        a, b = diagonal(c, q, level)
        other = swap(a)
        scale = w / (a * other + b * b)
        return other * scale, -b * scale

    for i in range(N2):
        w = weight(2 * my + i - 2 * REACH, 2 * slabs)
        for q in range(2):
            parts = invert_packed(c2[i], q, 2, w)
            d2[q, 0, i], d2[q, 1, i] = parts
    for i in range(N3):
        c = block_sum_spread(c2[2 * i + 2] + c2[2 * i + 3]) * np.float32(0.125)
        w = weight(my + i - (REACH - 1), slabs)
        for q in range(2):
            parts = invert_packed(c, q, 3, w)
            d3[q, 0, i], d3[q, 1, i] = parts

    def spread(src, dst, d, out_sem, in_sem):
        remote(src, dst, out_sem, in_sem, (me, slab(d)))

    for l in range(2):
        for q in range(2):
            four = pl.ds(4 * q, 4)
            landed(spec.at[pl.ds(0, 3), :, four, l], 2 + 2 * l + q)
            for a in range(TM):
                x = layer_of(a, l)
                here = g0.at[:, four, H0 + x]
                if x < H0:
                    spread(here, g0.at[:, four, H0 + LAYERS + x], -1, 4, 9 + q)
                if x >= LAYERS - H0:
                    spread(here, g0.at[:, four, x - (LAYERS - H0)], 1, 4, 9 + q)

    def jacobi(inverse, er, ei):
        a, b, c = inverse
        return a * er + b * ei, c * ei - b * er

    def sweep(level, below, here, above, g, inverse):
        er = g[0] - level.neighbours(below[0], here[0], above[0])
        ei = g[1] - level.neighbours(below[1], here[1], above[1])
        ur, ui = jacobi(inverse, er, ei)
        keep = np.float32(KEEP)
        return keep * here[0] + ur, keep * here[1] + ui

    def defect(level, below, here, above, g, c, shifts, six_here):
        first, second, third = shifts
        q = c * second
        er = g[0] - level.neighbours(below[0], here[0], above[0])
        ei = g[1] - level.neighbours(below[1], here[1], above[1])
        er = er - ((c * first + six_here) * here[0] - q * here[1])
        ei = ei - (q * here[0] + (c * third + six_here) * here[1])
        return er, ei

    def pre(level, count, own, load_g, load_d, load_c, shifts, six_here, keep_v, keep_r):
        once, twice, waiting = {}, {}, None
        for i in range(count):
            once[i] = jacobi(load_d(i), *load_g(i))
            if i < 2:
                continue
            j = i - 1
            twice[j] = sweep(level, once[j - 1], once[j], once[j + 1], load_g(j), load_d(j))
            keep_v(j, twice[j])
            j = i - 2
            if j - own[0] in range(own[1]):
                r = defect(
                    level,
                    twice[j - 1],
                    twice[j],
                    twice[j + 1],
                    load_g(j),
                    load_c(j),
                    shifts,
                    six_here,
                )
                if (j - own[0]) % 2:
                    keep_r((j - own[0]) // 2, (waiting[0] + r[0], waiting[1] + r[1]))
                waiting = r

    def post(level, first, count, load_v, load_g, load_d, keep):
        once = {}
        start = {}
        for i in range(first - 2, first + count + 2):
            start[i] = load_v(i)
            j = i - 1
            if j < first - 1:
                continue
            once[j] = sweep(level, start[j - 1], start[j], start[j + 1], load_g(j), load_d(j))
            j = i - 2
            if j < first:
                continue
            keep(j, sweep(level, once[j - 1], once[j], once[j + 1], load_g(j), load_d(j)))

    eighth = np.float32(0.125)
    level0 = Level(0, 8, 128)
    level1 = Level(1, 4, 64)
    level2 = Level(2, 2, 32)
    level3 = Level(3, 1, 32, 2)

    def down0(slot, carry):
        def keep_v(i, v):
            v0[slot, 0, i], v0[slot, 1, i] = v

        def keep_r(i, r):
            for c in range(2):
                small0[slot, c, i] = block_sum(r[c]) * eighth

        pre(
            level0,
            N0,
            (H0, LAYERS),
            lambda i: (g0[0, slot, i], g0[1, slot, i]),
            lambda i: tuple(d0[slot, k, i] for k in range(3)),
            lambda i: c0[i],
            tuple(tab[3 * slot + k] for k in range(3)),
            six[0],
            keep_v,
            keep_r,
        )
        return carry

    for q in range(2):
        landed(g0.at[:, pl.ds(4 * q, 4), pl.ds(0, 2 * H0)], 9 + q)
        lax.fori_loop(4 * q, 4 * q + 4, down0, 0)
        for c in range(2):
            for i in range(4):
                tiles = [[small0[4 * q + 2 * sb + lb, c, i] for lb in range(2)] for sb in range(2)]
                g1[q, c, H1 + i] = pack(tiles)
        mine = g1.at[q, :, pl.ds(H1, 4)]
        spread(mine, g1.at[q, :, pl.ds(H1 + 4, 4)], -1, 5, 11 + q)
        spread(mine, g1.at[q, :, pl.ds(0, 4)], 1, 5, 11 + q)

    for q in range(2):
        landed(g1.at[q, :, pl.ds(0, 8)], 11 + q)
        coarse = {}

        def keep_v(i, v, q=q):
            v1[q, 0, i], v1[q, 1, i] = v

        def keep_r(i, r, coarse=coarse):
            for c in range(2):
                coarse[c, i] = block_sum(r[c]) * eighth

        pre(
            level1,
            N1,
            (H1, 4),
            lambda i, q=q: (g1[q, 0, i], g1[q, 1, i]),
            lambda i, q=q: tuple(d1[q, k, i] for k in range(3)),
            lambda i: c1[i],
            tuple(tab[24 + 3 * q + k] for k in range(3)),
            six[1],
            keep_v,
            keep_r,
        )
        p2[q, REACH] = pack([[coarse[c, 0], coarse[c, 1]] for c in range(2)])
        for d in SHIFTS:
            spread(p2.at[q, REACH], p2.at[q, REACH - d], d, 6, 13 + q)

    def relax(d, q, i, e):
        return d[q, 0, i] * e + d[q, 1, i] * swap(e)

    def sweep_packed(level, below, here, above, g, d, q, i):
        return np.float32(KEEP) * here + relax(d, q, i, g - level.neighbours(below, here, above))

    def coarse_levels(q):
        for i in range(N2 // 2):
            g2[q, 2 * i], g2[q, 2 * i + 1] = p2[q, i], pltpu.roll(p2[q, i], 64, 1)
        for i in range(N2):
            w2[i] = relax(d2, q, i, g2[q, i])
        for i in range(1, N2 - 1):
            v2[i] = sweep_packed(level2, w2[i - 1], w2[i], w2[i + 1], g2[q, i], d2, q, i)
        right = []
        for m in range(N3):
            pair = []
            for i in (2 * m + 2, 2 * m + 3):
                here = v2[i]
                a, b = diagonal(c2[i], q, 2)
                pair.append(
                    g2[q, i]
                    - level2.neighbours(v2[i - 1], here, v2[i + 1])
                    - (a * here + b * swap(here))
                )
            right.append(block_sum_spread(pair[0] + pair[1]) * eighth)
        current = {m: relax(d3, q, m, right[m]) for m in range(N3)}
        for s in range(1, 6):
            current = {
                m: sweep_packed(
                    level3, current[m - 1], current[m], current[m + 1], right[m], d3, q, m
                )
                for m in range(s, N3 - s)
            }
        low = 2 * 5 + 2
        stage = {i: v2[i] + current[(i - 2) // 2] for i in range(low, low + 10)}
        for s in range(1, 3):
            stage = {
                i: sweep_packed(level2, stage[i - 1], stage[i], stage[i + 1], g2[q, i], d2, q, i)
                for i in range(low + s, low + 10 - s)
            }
        return stage

    def up1(q, stage):
        correction = {}

        def load_v(i):
            m = 2 * REACH + (i - H1) // 2
            if m not in correction:
                correction[m] = [unpack(stage[m], c, 0) for c in range(2)]
            return tuple(v1[q, c, i] + correction[m][c] for c in range(2))

        def keep(i, v):
            v1[q, 0, i], v1[q, 1, i] = v

        post(
            level1,
            H1 - 1,
            6,
            load_v,
            lambda i: (g1[q, 0, i], g1[q, 1, i]),
            lambda i: tuple(d1[q, k, i] for k in range(3)),
            keep,
        )

    def up0(q, k, carry):
        slot, sb, lb = 4 * q + k, k >> 1, k & 1
        correction = {}

        def load_v(i):
            m = H1 + (i - H0) // 2
            if m not in correction:
                correction[m] = [unpack(v1[q, c, m], sb, lb) for c in range(2)]
            return tuple(v0[slot, c, i] + correction[m][c] for c in range(2))

        def keep(i, v):
            solved[0, slot, i - H0], solved[1, slot, i - H0] = v

        post(
            level0,
            H0,
            LAYERS,
            load_v,
            lambda i: (g0[0, slot, i], g0[1, slot, i]),
            lambda i: tuple(d0[slot, k, i] for k in range(3)),
            keep,
        )
        return carry

    for q in range(2):
        landed(p2.at[q, pl.ds(0, 2 * REACH)], 13 + q)
        stage = coarse_levels(q)
        up1(q, stage)
        lax.fori_loop(0, 4, lambda k, carry, q=q: up0(q, k, carry), 0)
        four = pl.ds(4 * q, 4)
        for l in range(2):
            exchange(
                2,
                6 + l,
                lambda j, l=l, four=four: solved.at[:, four, layer_of(j, l)],
                back.at[me, :, four, l],
            )
        for l in range(2):
            for c in range(2):
                for slot in range(4 * q, 4 * q + 4):
                    back[me, c, slot, l] = solved[c, slot, layer_of(me, l)]

    def inverse(l):
        def field(j, slot, factor=2.0):
            return tuple(back[j, c, slot, l] * np.float32(factor) for c in range(2))

        nothing = (None, None)
        packed = field(0, 0, 1.0)
        line = [(packed[0], None)] + [field(0, m) for m in (1, 2, 3)] + [(packed[1], None)]
        line = transform(line + [nothing] * 3, 1.0)
        middle = [[(line[t2][0], None) for t2 in range(8)]]
        for k1 in (1, 2, 3):
            line = transform([field(k1, m) for m in range(8)], 1.0)
            middle.append(
                [twisted(line[t2], 2.0 * math.pi * k1 * t2 / LENGTH) for t2 in range(8)]
            )
        line = transform([field(0, 4 + m) for m in range(4)] + [nothing] * 4, 1.0)
        turned = [twisted(line[t2], 2.0 * math.pi * 4 * t2 / LENGTH) for t2 in range(8)]
        middle.append([(turned[t2][0], None) for t2 in range(8)])
        for t2 in range(8):
            column = transform([middle[k1][t2] for k1 in range(5)] + [nothing] * 3, 1.0)
            for t1 in range(8):
                t = 8 * t1 + t2
                values[l, t] = column[t1][0] * np.float32(BETA ** (-t) / LENGTH)

    for l in range(2):
        landed(back.at[pl.ds(0, 3), :, :, l], 6 + l)
        inverse(l)
        mine = out.at[:, layer_of(me, l)]
        exchange(3, 8, lambda j, l=l: values.at[l, pl.ds(16 * j, 16)], mine)
        for t in range(16):
            out[t, layer_of(me, l)] = values[l, 16 * me + t]
    sent(series.at[pl.ds(0, 48)], 0)
    sent(spec.at[pl.ds(0, 3)], 1)
    sent(back.at[pl.ds(0, 3)], 2)
    sent(g0.at[:, :, pl.ds(0, 2 * H0)], 4)
    sent(g1.at[:, :, pl.ds(0, 8)], 5)
    sent(p2.at[:, pl.ds(0, 2 * REACH)], 6)
    sent(series.at[pl.ds(0, 46), 0], 7)
    sent(values.at[:, pl.ds(0, 48)], 3)
    landed(values.at[:, pl.ds(0, 48)], 8)


def write_out(src, dst, sem):
    copy = pltpu.make_async_copy(src, dst, sem.at[0])
    copy.start()
    copy.wait()


def solution(mesh):
    slabs = mesh.shape["space"]
    table = shift_tables()

    def tiles(*lead):
        return pltpu.VMEM(lead + (8, 128), F32)

    def on_device(residual, capacity):
        any_space = pl.BlockSpec(memory_space=pl.ANY)
        dma = pltpu.SemaphoreType.DMA
        result = pl.pallas_call(
            lambda *refs: kernel(slabs, *refs),
            out_shape=jax.ShapeDtypeStruct(residual.shape, F32),
            in_specs=[any_space] * 3,
            out_specs=pl.BlockSpec(memory_space=pltpu.VMEM),
            scratch_shapes=[
                tiles(16, LAYERS),
                tiles(LAYERS),
                tiles(34),
                tiles(LENGTH, 2),
                tiles(TM, 2, SLOTS, 2),
                tiles(2, SLOTS, N0),
                tiles(SLOTS, 2, N0),
                tiles(N0),
                tiles(SLOTS, 3, N0),
                tiles(SLOTS, 2, 4),
                tiles(2, 2, N1),
                tiles(2, 2, N1),
                tiles(N1),
                tiles(2, 3, N1),
                tiles(2, N2),
                tiles(N2),
                tiles(N2),
                tiles(N2),
                tiles(2, 2, N2),
                tiles(2, 2, N3),
                tiles(2, SLOTS, LAYERS),
                tiles(TM, 2, SLOTS, 2),
                tiles(2, LENGTH),
                tiles(2, 1 + 2 * REACH),
                dma((3,)),
                dma((8,)),
                dma((16,)),
            ],
            compiler_params=pltpu.CompilerParams(collective_id=0, has_side_effects=True, vmem_limit_bytes=24 << 20),
            name="paradiag",
        )(*(pltpu.with_memory_space_constraint(v, pltpu.HBM) for v in (residual, capacity, jnp.asarray(table))))
        return pl.pallas_call(
            write_out,
            out_shape=jax.ShapeDtypeStruct(residual.shape, F32),
            in_specs=[pl.BlockSpec(memory_space=pltpu.VMEM)],
            out_specs=any_space,
            scratch_shapes=[dma((1,))],
            compiler_params=pltpu.CompilerParams(vmem_limit_bytes=1 << 20),
            name="write_out",
        )(result)

    return jax.shard_map(
        on_device,
        mesh=mesh,
        in_specs=(P("tm", "space", None, None), P("space", None, None)),
        out_specs=P("tm", "space", None, None),
        check_vma=False,
    )
```

```python
import math

import jax
import jax.numpy as jnp
import numpy as np
from jax import lax
from jax.experimental import pallas as pl
from jax.experimental.pallas import tpu as pltpu
from jax.sharding import PartitionSpec as P

MESH = pl.DeviceIdType.MESH
F32 = jnp.float32

ALPHA_CORNER = 0.01
STEP_SIZE = 0.5
DIFFUSE = 2.0
ADVECT = (0.2, -0.15, 0.1)
OMEGA = 0.7
KEEP = 1.0 - OMEGA
LENGTH = 64
BETA = ALPHA_CORNER ** (1.0 / LENGTH)

TM = 4
SLOTS = 8
LAYERS = 8
H0 = 3
H1 = 4
REACH = 8
N0 = LAYERS + 2 * H0
N1 = LAYERS // 2 + 2 * H1
N2 = LAYERS // 4 * (1 + 2 * REACH)
N3 = N2 // 2 - 2
SHIFTS = [d for k in (4, 5, 3, 6, 2, 7, 8, 1) for d in (k, -k)]

FREQUENCIES = [[0, 8, 16, 24, 4, 12, 20, 28]] + [[k + 8 * m for m in range(8)] for k in (1, 2, 3)]


def shift_tables():
    table = np.zeros((TM, 34, 8, 128), np.float64)
    for a in range(TM):
        one, two, three = [], [], []
        for slot in range(SLOTS):
            phase = 2.0 * math.pi * FREQUENCIES[a][slot] / LENGTH
            first = (1.0 - BETA * math.cos(phase)) / STEP_SIZE
            second = BETA * math.sin(phase) / STEP_SIZE
            third = first
            if a == 0 and slot == 0:
                second, third = 0.0, (1.0 + BETA) / STEP_SIZE
            one.append(first)
            two.append(second)
            three.append(third)
        for slot in range(SLOTS):
            for c, values in enumerate((one, two, three)):
                table[a, 3 * slot + c] = values[slot]
                q, sb, lb = slot // 4, slot // 2 % 2, slot % 2
                table[a, 24 + 3 * q + c, 4 * sb : 4 * sb + 4, 64 * lb : 64 * lb + 64] = values[slot]
            for lanes in (slice(32 * lb, 32 * lb + 32), slice(64 + 32 * lb, 96 + 32 * lb)):
                table[a, 30 + 2 * q, 2 * sb : 2 * sb + 2, lanes] = one[slot]
                table[a, 30 + 2 * q, 4 + 2 * sb : 6 + 2 * sb, lanes] = three[slot]
                table[a, 31 + 2 * q, 2 * sb : 2 * sb + 2, lanes] = -two[slot]
                table[a, 31 + 2 * q, 4 + 2 * sb : 6 + 2 * sb, lanes] = two[slot]
    return table.astype(np.float32)


def plus(a, b):
    return b if a is None else a if b is None else a + b


def minus(a, b):
    return a if b is None else -b if a is None else a - b


def scaled(a, factor):
    if a is None or abs(factor) < 1e-15:
        return None
    if abs(factor - 1.0) < 1e-15:
        return a
    if abs(factor + 1.0) < 1e-15:
        return -a
    return a * np.float32(factor)


def twisted(value, phase):
    c, s = math.cos(phase), math.sin(phase)
    re, im = value
    return (minus(scaled(re, c), scaled(im, s)), plus(scaled(re, s), scaled(im, c)))


def transform(values, sign):
    n = len(values)
    if n == 1:
        return values
    even = transform(values[0::2], sign)
    odd = transform(values[1::2], sign)
    upper, lower = [], []
    for k in range(n // 2):
        turned = twisted(odd[k], sign * 2.0 * math.pi * k / n)
        upper.append((plus(even[k][0], turned[0]), plus(even[k][1], turned[1])))
        lower.append((minus(even[k][0], turned[0]), minus(even[k][1], turned[1])))
    return upper + lower


def rows_lanes():
    return (
        lax.broadcasted_iota(jnp.int32, (8, 128), 0),
        lax.broadcasted_iota(jnp.int32, (8, 128), 1),
    )


class Level:
    def __init__(self, level, ny, nz, step=1):
        row, lane = rows_lanes()
        self.spread = DIFFUSE / 4.0**level
        bx, by, bz = (b / 2.0**level for b in ADVECT)
        c = self.spread
        self.xp, self.xm = np.float32(-c + bx), np.float32(-c - bx)
        self.step = step
        self.ny = ny
        zero = jnp.zeros((8, 128), F32)
        y, z = row % 8 % max(ny, 1), lane % nz
        if ny > 1:
            self.yp = jnp.where(y < ny - 1, np.float32(-c + by), zero)
            self.ym = jnp.where(y > 0, np.float32(-c - by), zero)
        self.zp = jnp.where(z < nz - step, np.float32(-c + bz), zero)
        self.zm = jnp.where(z >= step, np.float32(-c - bz), zero)

    def neighbours(self, below, here, above):
        total = self.xp * above + self.xm * below
        total += self.zp * pltpu.roll(here, 128 - self.step, 1)
        total += self.zm * pltpu.roll(here, self.step, 1)
        if self.ny > 1:
            total += self.yp * pltpu.roll(here, 7, 0)
            total += self.ym * pltpu.roll(here, 1, 0)
        return total


def block_sum(value):
    value = value + pltpu.roll(value, 7, 0)
    return value + pltpu.roll(value, 127, 1)


def block_sum_spread(value):
    row, lane = rows_lanes()
    value = value + jnp.where(row % 2 == 0, pltpu.roll(value, 7, 0), pltpu.roll(value, 1, 0))
    return value + jnp.where(lane % 2 == 0, pltpu.roll(value, 127, 1), pltpu.roll(value, 1, 1))


def take(value, index, axis):
    return jnp.take_along_axis(value, index, axis=axis, mode="promise_in_bounds")


def pack(tiles):
    row, lane = rows_lanes()
    even_lane, even_row = lane * 2 % 128, row * 2 % 8
    halves = []
    for left, right in tiles:
        if left is right:
            halves.append(take(left, even_lane, 1))
        else:
            halves.append(jnp.where(lane < 64, take(left, even_lane, 1), take(right, even_lane, 1)))
    if tiles[0] is tiles[1]:
        return take(halves[0], even_row, 0)
    return jnp.where(row < 4, take(halves[0], even_row, 0), take(halves[1], even_row, 0))


def unpack(tile, rb, lb):
    row, lane = rows_lanes()
    return take(take(tile, 4 * rb + row // 2, 0), 64 * lb + lane // 2, 1)


def layer_of(a, l):
    return 2 * a + l + (a // 2) * (1 - 2 * l)


def kernel(
    slabs,
    res_in,
    cap_in,
    tab_in,
    out,
    res,
    cap,
    tab,
    series,
    spec,
    g0,
    v0,
    c0,
    d0,
    small0,
    g1,
    v1,
    c1,
    d1,
    g2,
    w2,
    v2,
    c2,
    d2,
    d3,
    solved,
    back,
    values,
    p2,
    o0,
    local_sem,
    send_sem,
    recv_sem,
):
    me, my = lax.axis_index("tm"), lax.axis_index("space")

    def peer(d):
        return lax.rem(me + d, TM)

    def slab(d):
        return lax.rem(my + (d + 8 * slabs), slabs)

    def local(src, dst, n):
        copy = pltpu.make_async_copy(src, dst, local_sem.at[n])
        copy.start()
        return copy.wait

    res_wait = local(res_in, res, 0)
    cap_wait = local(cap_in, cap, 1)
    table_wait = local(tab_in.at[me], tab, 2)

    barrier = pltpu.get_barrier_semaphore()
    greeted = 0
    for d in range(1, TM):
        pl.semaphore_signal(barrier, inc=1, device_id=(peer(d), my), device_id_type=MESH)
        greeted += 1
    for d in SHIFTS:
        if d % slabs:
            pl.semaphore_signal(barrier, inc=1, device_id=(me, slab(d)), device_id_type=MESH)
            greeted += 1
    pl.semaphore_wait(barrier, greeted)

    def remote(src, dst, out_sem, in_sem, device):
        pltpu.make_async_remote_copy(
            src_ref=src,
            dst_ref=dst,
            send_sem=send_sem.at[out_sem],
            recv_sem=recv_sem.at[in_sem],
            device_id=device,
            device_id_type=MESH,
        ).start()

    def landed(size, n):
        pltpu.make_async_copy(size, size, recv_sem.at[n]).wait()

    def sent(size, n):
        pltpu.make_async_copy(size, size, send_sem.at[n]).wait()

    def exchange(out_sem, in_sem, source, target):
        for d in (2, 1, 3):
            remote(source(peer(d)), target, out_sem, in_sem, (peer(d), my))

    res_wait()
    for l in range(2):
        exchange(
            0,
            0 + l,
            lambda j, l=l: res.at[:, layer_of(j, l)],
            series.at[pl.ds(16 * me, 16), l],
        )
    for l in range(2):
        for t in range(16):
            series[16 * me + t, l] = res[t, layer_of(me, l)]

    cap_wait()

    def spread_cap(src, dst, d):
        remote(src, dst, 7, 15, (me, slab(d)))

    spread_cap(cap.at[pl.ds(0, H0)], c0.at[pl.ds(H0 + LAYERS, H0)], -1)
    spread_cap(cap.at[pl.ds(LAYERS - H0, H0)], c0.at[pl.ds(0, H0)], 1)
    for i in range(LAYERS):
        c0[H0 + i] = cap[i]
    for i in range(LAYERS // 2):
        tile = block_sum(cap[2 * i] + cap[2 * i + 1]) * np.float32(0.125)
        c1[H1 + i] = pack(((tile, tile),) * 2)
    spread_cap(c1.at[pl.ds(H1, 4)], c1.at[pl.ds(H1 + 4, 4)], -1)
    spread_cap(c1.at[pl.ds(H1, 4)], c1.at[pl.ds(0, 4)], 1)
    for i in range(LAYERS // 4):
        tile = block_sum(c1[H1 + 2 * i] + c1[H1 + 2 * i + 1]) * np.float32(0.125)
        c2[2 * REACH + i] = pack(((tile, tile),) * 2)
    for d in SHIFTS:
        spread_cap(c2.at[pl.ds(2 * REACH, 2)], c2.at[pl.ds(2 * (REACH - d), 2)], d)

    def forward(l):
        middle = [[None] * 8 for _ in range(5)]
        for t2 in range(8):
            column = [
                (series[8 * t1 + t2, l] * np.float32(BETA ** (8 * t1 + t2)), None)
                for t1 in range(8)
            ]
            first = transform(column, -1.0)
            for k1 in range(5):
                middle[k1][t2] = twisted(first[k1], -2.0 * math.pi * k1 * t2 / LENGTH)
        for k1 in range(5):
            last = transform(middle[k1], -1.0)
            if k1 == 0:
                spec[0, 0, 0, l], spec[0, 1, 0, l] = last[0][0], last[4][0]
                chosen = [(m, 0, m) for m in (1, 2, 3)]
            elif k1 == 4:
                chosen = [(m, 0, 4 + m) for m in range(4)]
            else:
                chosen = [(m, k1, m) for m in range(8)]
            for m, j, slot in chosen:
                spec[j, 0, slot, l], spec[j, 1, slot, l] = last[m]

    for l in range(2):
        landed(series.at[pl.ds(0, 48), l], l)
        forward(l)
        for q in range(2):
            four = pl.ds(4 * q, 4)
            exchange(
                1,
                2 + 2 * l + q,
                lambda j, l=l, four=four: spec.at[j, :, four, l],
                g0.at[:, four, H0 + layer_of(me, l)],
            )
        here = H0 + layer_of(me, l)
        for c in range(2):
            for slot in range(SLOTS):
                g0[c, slot, here] = spec[me, c, slot, l]

    table_wait()
    landed(series.at[pl.ds(0, 46), 0], 15)

    def weight(index, extent):
        inside = jnp.logical_and(index >= 0, index < extent)
        return jnp.where(inside, np.float32(OMEGA), np.float32(0.0))

    six = [np.float32(6.0 * DIFFUSE / 4.0**level) for level in range(4)]

    def invert(c, first, second, third, diagonal, w):
        top, q, bottom = c * first + diagonal, c * second, c * third + diagonal
        scale = w / (top * bottom + q * q)
        return bottom * scale, q * scale, top * scale

    def invert0(slot, carry):
        first, second, third = (tab[3 * slot + k] for k in range(3))
        for i in range(N0):
            w = weight(LAYERS * my + i - H0, LAYERS * slabs)
            parts = invert(c0[i], first, second, third, six[0], w)
            for k in range(3):
                d0[slot, k, i] = parts[k]
        return carry

    lax.fori_loop(0, SLOTS, invert0, 0)
    for q in range(2):
        first, second, third = (tab[24 + 3 * q + k] for k in range(3))
        for i in range(N1):
            w = weight(4 * my + i - H1, 4 * slabs)
            parts = invert(c1[i], first, second, third, six[1], w)
            for k in range(3):
                d1[q, k, i] = parts[k]

    def diagonal(c, q, level):
        return c * tab[30 + 2 * q] + six[level], c * tab[31 + 2 * q]

    def swap(value):
        return pltpu.roll(value, 4, 0)

    def invert_packed(c, q, level, w):
        a, b = diagonal(c, q, level)
        other = swap(a)
        scale = w / (a * other + b * b)
        return other * scale, -b * scale

    for i in range(N2):
        w = weight(2 * my + i - 2 * REACH, 2 * slabs)
        for q in range(2):
            parts = invert_packed(c2[i], q, 2, w)
            d2[q, 0, i], d2[q, 1, i] = parts
    for i in range(N3):
        c = block_sum_spread(c2[2 * i + 2] + c2[2 * i + 3]) * np.float32(0.125)
        w = weight(my + i - (REACH - 1), slabs)
        for q in range(2):
            parts = invert_packed(c, q, 3, w)
            d3[q, 0, i], d3[q, 1, i] = parts

    def spread(src, dst, d, out_sem, in_sem):
        remote(src, dst, out_sem, in_sem, (me, slab(d)))

    for l in range(2):
        for q in range(2):
            four = pl.ds(4 * q, 4)
            landed(spec.at[pl.ds(0, 3), :, four, l], 2 + 2 * l + q)
            for a in range(TM):
                x = layer_of(a, l)
                here = g0.at[:, four, H0 + x]
                if x < H0:
                    spread(here, g0.at[:, four, H0 + LAYERS + x], -1, 4, 9 + q)
                if x >= LAYERS - H0:
                    spread(here, g0.at[:, four, x - (LAYERS - H0)], 1, 4, 9 + q)

    def jacobi(inverse, er, ei):
        a, b, c = inverse
        return a * er + b * ei, c * ei - b * er

    def sweep(level, below, here, above, g, inverse):
        er = g[0] - level.neighbours(below[0], here[0], above[0])
        ei = g[1] - level.neighbours(below[1], here[1], above[1])
        ur, ui = jacobi(inverse, er, ei)
        keep = np.float32(KEEP)
        return keep * here[0] + ur, keep * here[1] + ui

    def defect(level, below, here, above, g, c, shifts, six_here):
        first, second, third = shifts
        q = c * second
        er = g[0] - level.neighbours(below[0], here[0], above[0])
        ei = g[1] - level.neighbours(below[1], here[1], above[1])
        er = er - ((c * first + six_here) * here[0] - q * here[1])
        ei = ei - (q * here[0] + (c * third + six_here) * here[1])
        return er, ei

    def pre(level, count, own, load_g, load_d, load_c, shifts, six_here, keep_v, keep_r):
        once, twice, waiting = {}, {}, None
        for i in range(count):
            once[i] = jacobi(load_d(i), *load_g(i))
            if i < 2:
                continue
            j = i - 1
            twice[j] = sweep(level, once[j - 1], once[j], once[j + 1], load_g(j), load_d(j))
            keep_v(j, twice[j])
            j = i - 2
            if j - own[0] in range(own[1]):
                r = defect(
                    level,
                    twice[j - 1],
                    twice[j],
                    twice[j + 1],
                    load_g(j),
                    load_c(j),
                    shifts,
                    six_here,
                )
                if (j - own[0]) % 2:
                    keep_r((j - own[0]) // 2, (waiting[0] + r[0], waiting[1] + r[1]))
                waiting = r

    def post(level, first, count, load_v, load_g, load_d, keep):
        once = {}
        start = {}
        for i in range(first - 2, first + count + 2):
            start[i] = load_v(i)
            j = i - 1
            if j < first - 1:
                continue
            once[j] = sweep(level, start[j - 1], start[j], start[j + 1], load_g(j), load_d(j))
            j = i - 2
            if j < first:
                continue
            keep(j, sweep(level, once[j - 1], once[j], once[j + 1], load_g(j), load_d(j)))

    eighth = np.float32(0.125)
    level0 = Level(0, 8, 128)
    level1 = Level(1, 4, 64)
    level2 = Level(2, 2, 32)
    level3 = Level(3, 1, 32, 2)

    def looped(start, count, together, body):
        def some(n, carry):
            for k in range(together):
                body(start + n * together + k, carry)
            return carry

        if together == count:
            some(0, 0)
        else:
            lax.fori_loop(0, count // together, some, 0)

    def views0(slot):
        return (
            lambda i: (g0[0, slot, i], g0[1, slot, i]),
            lambda i: tuple(d0[slot, k, i] for k in range(3)),
        )

    def keep0(slot, i, v):
        v0[slot, 0, i], v0[slot, 1, i] = v

    def coarsen0(slot, twice, layers, load_g):
        shifts = tuple(tab[3 * slot + k] for k in range(3))
        for i in layers:
            pair = [
                defect(
                    level0, twice[j - 1], twice[j], twice[j + 1], load_g(j), c0[j], shifts, six[0]
                )
                for j in (i, i + 1)
            ]
            for c in range(2):
                small0[slot, c, (i - H0) // 2] = block_sum(pair[0][c] + pair[1][c]) * eighth

    first, last = H0, H0 + LAYERS - 1

    def inside0(slot, carry):
        load_g, load_d = views0(slot)
        once, twice = {}, {}
        for i in range(first, last + 1):
            once[i] = jacobi(load_d(i), *load_g(i))
            if i - 2 >= first:
                j = i - 1
                twice[j] = sweep(level0, once[j - 1], once[j], once[j + 1], load_g(j), load_d(j))
                keep0(slot, j, twice[j])
        for n, i in enumerate((first, first + 1, last - 1, last)):
            o0[slot, 0, n], o0[slot, 1, n] = once[i]
        coarsen0(slot, twice, range(first + 2, last - 2, 2), load_g)
        return carry

    def outside0(slot, carry):
        load_g, load_d = views0(slot)
        for edge, step, stored in ((first, -1, (0, 1)), (last, 1, (3, 2))):
            once = {
                edge: (o0[slot, 0, stored[0]], o0[slot, 1, stored[0]]),
                edge - step: (o0[slot, 0, stored[1]], o0[slot, 1, stored[1]]),
            }
            twice = {
                i: (v0[slot, 0, i], v0[slot, 1, i]) for i in (edge - step, edge - 2 * step)
            }
            for n in range(1, H0 + 1):
                i = edge + n * step
                once[i] = jacobi(load_d(i), *load_g(i))
                j = i - step
                twice[j] = sweep(level0, once[j - 1], once[j], once[j + 1], load_g(j), load_d(j))
                keep0(slot, j, twice[j])
            coarsen0(slot, twice, (min(edge, edge - step),), load_g)
        return carry

    for q in range(2):
        looped(4 * q, 4, 4, inside0)

    for q in range(2):
        landed(g0.at[:, pl.ds(4 * q, 4), pl.ds(0, 2 * H0)], 9 + q)
        looped(4 * q, 4, 4, outside0)
        for c in range(2):
            for i in range(4):
                tiles = [[small0[4 * q + 2 * sb + lb, c, i] for lb in range(2)] for sb in range(2)]
                g1[q, c, H1 + i] = pack(tiles)
        mine = g1.at[q, :, pl.ds(H1, 4)]
        spread(mine, g1.at[q, :, pl.ds(H1 + 4, 4)], -1, 5, 11 + q)
        spread(mine, g1.at[q, :, pl.ds(0, 4)], 1, 5, 11 + q)

    for q in range(2):
        landed(g1.at[q, :, pl.ds(0, 8)], 11 + q)
        coarse = {}

        def keep_v(i, v, q=q):
            v1[q, 0, i], v1[q, 1, i] = v

        def keep_r(i, r, coarse=coarse):
            for c in range(2):
                coarse[c, i] = block_sum(r[c]) * eighth

        pre(
            level1,
            N1,
            (H1, 4),
            lambda i, q=q: (g1[q, 0, i], g1[q, 1, i]),
            lambda i, q=q: tuple(d1[q, k, i] for k in range(3)),
            lambda i: c1[i],
            tuple(tab[24 + 3 * q + k] for k in range(3)),
            six[1],
            keep_v,
            keep_r,
        )
        p2[q, REACH] = pack([[coarse[c, 0], coarse[c, 1]] for c in range(2)])
        for d in SHIFTS:
            spread(p2.at[q, REACH], p2.at[q, REACH - d], d, 6, 13 + q)

    def relax(d, q, i, e):
        return d[q, 0, i] * e + d[q, 1, i] * swap(e)

    def sweep_packed(level, below, here, above, g, d, q, i):
        return np.float32(KEEP) * here + relax(d, q, i, g - level.neighbours(below, here, above))

    def coarse_levels(q):
        for i in range(N2 // 2):
            g2[q, 2 * i], g2[q, 2 * i + 1] = p2[q, i], pltpu.roll(p2[q, i], 64, 1)
        for i in range(N2):
            w2[i] = relax(d2, q, i, g2[q, i])
        for i in range(1, N2 - 1):
            v2[i] = sweep_packed(level2, w2[i - 1], w2[i], w2[i + 1], g2[q, i], d2, q, i)
        right = []
        for m in range(N3):
            pair = []
            for i in (2 * m + 2, 2 * m + 3):
                here = v2[i]
                a, b = diagonal(c2[i], q, 2)
                pair.append(
                    g2[q, i]
                    - level2.neighbours(v2[i - 1], here, v2[i + 1])
                    - (a * here + b * swap(here))
                )
            right.append(block_sum_spread(pair[0] + pair[1]) * eighth)
        current = {m: relax(d3, q, m, right[m]) for m in range(N3)}
        for s in range(1, 6):
            current = {
                m: sweep_packed(
                    level3, current[m - 1], current[m], current[m + 1], right[m], d3, q, m
                )
                for m in range(s, N3 - s)
            }
        low = 2 * 5 + 2
        stage = {i: v2[i] + current[(i - 2) // 2] for i in range(low, low + 10)}
        for s in range(1, 3):
            stage = {
                i: sweep_packed(level2, stage[i - 1], stage[i], stage[i + 1], g2[q, i], d2, q, i)
                for i in range(low + s, low + 10 - s)
            }
        return stage

    def up1(q, stage):
        correction = {}

        def load_v(i):
            m = 2 * REACH + (i - H1) // 2
            if m not in correction:
                correction[m] = [unpack(stage[m], c, 0) for c in range(2)]
            return tuple(v1[q, c, i] + correction[m][c] for c in range(2))

        def keep(i, v):
            v1[q, 0, i], v1[q, 1, i] = v

        post(
            level1,
            H1 - 1,
            6,
            load_v,
            lambda i: (g1[q, 0, i], g1[q, 1, i]),
            lambda i: tuple(d1[q, k, i] for k in range(3)),
            keep,
        )

    def up0(q, k, carry):
        slot, sb, lb = 4 * q + k, k >> 1, k & 1
        correction = {}

        def load_v(i):
            m = H1 + (i - H0) // 2
            if m not in correction:
                correction[m] = [unpack(v1[q, c, m], sb, lb) for c in range(2)]
            return tuple(v0[slot, c, i] + correction[m][c] for c in range(2))

        def keep(i, v):
            solved[0, slot, i - H0], solved[1, slot, i - H0] = v

        post(
            level0,
            H0,
            LAYERS,
            load_v,
            lambda i: (g0[0, slot, i], g0[1, slot, i]),
            lambda i: tuple(d0[slot, k, i] for k in range(3)),
            keep,
        )
        return carry

    for q in range(2):
        landed(p2.at[q, pl.ds(0, 2 * REACH)], 13 + q)
        stage = coarse_levels(q)
        up1(q, stage)
        for k, size in ((0, 2), (2, 2)) if q == 0 else ((0, 4),):
            looped(k, size, 2, lambda k, carry, q=q: up0(q, k, carry))
            some = pl.ds(4 * q + k, size)
            for l in range(2):
                exchange(
                    2,
                    6 + l,
                    lambda j, l=l, some=some: solved.at[:, some, layer_of(j, l)],
                    back.at[me, :, some, l],
                )
        for l in range(2):
            for c in range(2):
                for slot in range(4 * q, 4 * q + 4):
                    back[me, c, slot, l] = solved[c, slot, layer_of(me, l)]

    def inverse(l):
        def field(j, slot, factor=2.0):
            return tuple(back[j, c, slot, l] * np.float32(factor) for c in range(2))

        nothing = (None, None)
        packed = field(0, 0, 1.0)
        line = [(packed[0], None)] + [field(0, m) for m in (1, 2, 3)] + [(packed[1], None)]
        line = transform(line + [nothing] * 3, 1.0)
        middle = [[(line[t2][0], None) for t2 in range(8)]]
        for k1 in (1, 2, 3):
            line = transform([field(k1, m) for m in range(8)], 1.0)
            middle.append(
                [twisted(line[t2], 2.0 * math.pi * k1 * t2 / LENGTH) for t2 in range(8)]
            )
        line = transform([field(0, 4 + m) for m in range(4)] + [nothing] * 4, 1.0)
        turned = [twisted(line[t2], 2.0 * math.pi * 4 * t2 / LENGTH) for t2 in range(8)]
        middle.append([(turned[t2][0], None) for t2 in range(8)])
        for t2 in range(8):
            column = transform([middle[k1][t2] for k1 in range(5)] + [nothing] * 3, 1.0)
            for t1 in range(8):
                t = 8 * t1 + t2
                values[l, t] = column[t1][0] * np.float32(BETA ** (-t) / LENGTH)

    for l in range(2):
        landed(back.at[pl.ds(0, 3), :, :, l], 6 + l)
        inverse(l)
        mine = out.at[:, layer_of(me, l)]
        exchange(3, 8, lambda j, l=l: values.at[l, pl.ds(16 * j, 16)], mine)
        for t in range(16):
            out[t, layer_of(me, l)] = values[l, 16 * me + t]
    sent(series.at[pl.ds(0, 48)], 0)
    sent(spec.at[pl.ds(0, 3)], 1)
    sent(back.at[pl.ds(0, 3)], 2)
    sent(g0.at[:, :, pl.ds(0, 2 * H0)], 4)
    sent(g1.at[:, :, pl.ds(0, 8)], 5)
    sent(p2.at[:, pl.ds(0, 2 * REACH)], 6)
    sent(series.at[pl.ds(0, 46), 0], 7)
    sent(values.at[:, pl.ds(0, 48)], 3)
    landed(values.at[:, pl.ds(0, 48)], 8)


def write_out(src, dst, sem):
    copy = pltpu.make_async_copy(src, dst, sem.at[0])
    copy.start()
    copy.wait()


def solution(mesh):
    slabs = mesh.shape["space"]
    table = shift_tables()

    def tiles(*lead):
        return pltpu.VMEM(lead + (8, 128), F32)

    def on_device(residual, capacity):
        any_space = pl.BlockSpec(memory_space=pl.ANY)
        dma = pltpu.SemaphoreType.DMA
        result = pl.pallas_call(
            lambda *refs: kernel(slabs, *refs),
            out_shape=jax.ShapeDtypeStruct(residual.shape, F32),
            in_specs=[any_space] * 3,
            out_specs=pl.BlockSpec(memory_space=pltpu.VMEM),
            scratch_shapes=[
                tiles(16, LAYERS),
                tiles(LAYERS),
                tiles(34),
                tiles(LENGTH, 2),
                tiles(TM, 2, SLOTS, 2),
                tiles(2, SLOTS, N0),
                tiles(SLOTS, 2, N0),
                tiles(N0),
                tiles(SLOTS, 3, N0),
                tiles(SLOTS, 2, 4),
                tiles(2, 2, N1),
                tiles(2, 2, N1),
                tiles(N1),
                tiles(2, 3, N1),
                tiles(2, N2),
                tiles(N2),
                tiles(N2),
                tiles(N2),
                tiles(2, 2, N2),
                tiles(2, 2, N3),
                tiles(2, SLOTS, LAYERS),
                tiles(TM, 2, SLOTS, 2),
                tiles(2, LENGTH),
                tiles(2, 1 + 2 * REACH),
                tiles(SLOTS, 2, 4),
                dma((3,)),
                dma((8,)),
                dma((16,)),
            ],
            compiler_params=pltpu.CompilerParams(collective_id=0, has_side_effects=True, vmem_limit_bytes=24 << 20),
            name="paradiag",
        )(*(pltpu.with_memory_space_constraint(v, pltpu.HBM) for v in (residual, capacity, jnp.asarray(table))))
        return pl.pallas_call(
            write_out,
            out_shape=jax.ShapeDtypeStruct(residual.shape, F32),
            in_specs=[pl.BlockSpec(memory_space=pltpu.VMEM)],
            out_specs=any_space,
            scratch_shapes=[dma((1,))],
            compiler_params=pltpu.CompilerParams(vmem_limit_bytes=1 << 20),
            name="write_out",
        )(result)

    return jax.shard_map(
        on_device,
        mesh=mesh,
        in_specs=(P("tm", "space", None, None), P("space", None, None)),
        out_specs=P("tm", "space", None, None),
        check_vma=False,
    )
```

```python
import math

import jax
import jax.numpy as jnp
import numpy as np
from jax import lax
from jax.experimental import pallas as pl
from jax.experimental.pallas import tpu as pltpu
from jax.sharding import PartitionSpec as P

MESH = pl.DeviceIdType.MESH
F32 = jnp.float32

ALPHA_CORNER = 0.01
STEP_SIZE = 0.5
DIFFUSE = 2.0
ADVECT = (0.2, -0.15, 0.1)
OMEGA = 0.7
KEEP = 1.0 - OMEGA
LENGTH = 64
BETA = ALPHA_CORNER ** (1.0 / LENGTH)

TM = 4
SLOTS = 8
LAYERS = 8
H0 = 6
H1 = 4
OWN1 = 2
REACH = 8
N0 = LAYERS + 2 * H0
N1 = LAYERS // 2 + 2 * H1
N2 = LAYERS // 4 * (1 + 2 * REACH)
N3 = N2 // 2 - 2
SHIFTS = [d for k in (4, 5, 3, 6, 2, 7, 8, 1) for d in (k, -k)]

FREQUENCIES = [[0, 8, 16, 24, 4, 12, 20, 28]] + [[k + 8 * m for m in range(8)] for k in (1, 2, 3)]


def shift_tables():
    table = np.zeros((TM, 34, 8, 128), np.float64)
    for a in range(TM):
        one, two, three = [], [], []
        for slot in range(SLOTS):
            phase = 2.0 * math.pi * FREQUENCIES[a][slot] / LENGTH
            first = (1.0 - BETA * math.cos(phase)) / STEP_SIZE
            second = BETA * math.sin(phase) / STEP_SIZE
            third = first
            if a == 0 and slot == 0:
                second, third = 0.0, (1.0 + BETA) / STEP_SIZE
            one.append(first)
            two.append(second)
            three.append(third)
        for slot in range(SLOTS):
            for c, values in enumerate((one, two, three)):
                table[a, 3 * slot + c] = values[slot]
                q, sb, lb = slot // 4, slot // 2 % 2, slot % 2
                table[a, 24 + 3 * q + c, 4 * sb : 4 * sb + 4, 64 * lb : 64 * lb + 64] = values[slot]
            for lanes in (slice(32 * lb, 32 * lb + 32), slice(64 + 32 * lb, 96 + 32 * lb)):
                table[a, 30 + 2 * q, 2 * sb : 2 * sb + 2, lanes] = one[slot]
                table[a, 30 + 2 * q, 4 + 2 * sb : 6 + 2 * sb, lanes] = three[slot]
                table[a, 31 + 2 * q, 2 * sb : 2 * sb + 2, lanes] = -two[slot]
                table[a, 31 + 2 * q, 4 + 2 * sb : 6 + 2 * sb, lanes] = two[slot]
    return table.astype(np.float32)


def plus(a, b):
    return b if a is None else a if b is None else a + b


def minus(a, b):
    return a if b is None else -b if a is None else a - b


def scaled(a, factor):
    if a is None or abs(factor) < 1e-15:
        return None
    if abs(factor - 1.0) < 1e-15:
        return a
    if abs(factor + 1.0) < 1e-15:
        return -a
    return a * np.float32(factor)


def twisted(value, phase):
    c, s = math.cos(phase), math.sin(phase)
    re, im = value
    return (minus(scaled(re, c), scaled(im, s)), plus(scaled(re, s), scaled(im, c)))


def transform(values, sign):
    n = len(values)
    if n == 1:
        return values
    even = transform(values[0::2], sign)
    odd = transform(values[1::2], sign)
    upper, lower = [], []
    for k in range(n // 2):
        turned = twisted(odd[k], sign * 2.0 * math.pi * k / n)
        upper.append((plus(even[k][0], turned[0]), plus(even[k][1], turned[1])))
        lower.append((minus(even[k][0], turned[0]), minus(even[k][1], turned[1])))
    return upper + lower


def rows_lanes():
    return (
        lax.broadcasted_iota(jnp.int32, (8, 128), 0),
        lax.broadcasted_iota(jnp.int32, (8, 128), 1),
    )


class Level:
    def __init__(self, level, ny, nz, step=1):
        row, lane = rows_lanes()
        self.spread = DIFFUSE / 4.0**level
        bx, by, bz = (b / 2.0**level for b in ADVECT)
        c = self.spread
        self.xp, self.xm = np.float32(-c + bx), np.float32(-c - bx)
        self.step = step
        self.ny = ny
        zero = jnp.zeros((8, 128), F32)
        y, z = row % 8 % max(ny, 1), lane % nz
        if ny > 1:
            self.yp = jnp.where(y < ny - 1, np.float32(-c + by), zero)
            self.ym = jnp.where(y > 0, np.float32(-c - by), zero)
        self.zp = jnp.where(z < nz - step, np.float32(-c + bz), zero)
        self.zm = jnp.where(z >= step, np.float32(-c - bz), zero)

    def neighbours(self, below, here, above):
        total = self.xp * above + self.xm * below
        total += self.zp * pltpu.roll(here, 128 - self.step, 1)
        total += self.zm * pltpu.roll(here, self.step, 1)
        if self.ny > 1:
            total += self.yp * pltpu.roll(here, 7, 0)
            total += self.ym * pltpu.roll(here, 1, 0)
        return total


def block_sum(value):
    value = value + pltpu.roll(value, 7, 0)
    return value + pltpu.roll(value, 127, 1)


def block_sum_spread(value):
    row, lane = rows_lanes()
    value = value + jnp.where(row % 2 == 0, pltpu.roll(value, 7, 0), pltpu.roll(value, 1, 0))
    return value + jnp.where(lane % 2 == 0, pltpu.roll(value, 127, 1), pltpu.roll(value, 1, 1))


def take(value, index, axis):
    return jnp.take_along_axis(value, index, axis=axis, mode="promise_in_bounds")


def pack(tiles):
    row, lane = rows_lanes()
    even_lane, even_row = lane * 2 % 128, row * 2 % 8
    halves = []
    for left, right in tiles:
        if left is right:
            halves.append(take(left, even_lane, 1))
        else:
            halves.append(jnp.where(lane < 64, take(left, even_lane, 1), take(right, even_lane, 1)))
    if tiles[0] is tiles[1]:
        return take(halves[0], even_row, 0)
    return jnp.where(row < 4, take(halves[0], even_row, 0), take(halves[1], even_row, 0))


def unpack(tile, rb, lb):
    row, lane = rows_lanes()
    return take(take(tile, 4 * rb + row // 2, 0), 64 * lb + lane // 2, 1)


def layer_of(a, l):
    return 2 * a + l + (a // 2) * (1 - 2 * l)


def kernel(
    slabs,
    res_in,
    cap_in,
    tab_in,
    out,
    res,
    cap,
    tab,
    series,
    spec,
    g0,
    v0,
    c0,
    d0,
    small0,
    g1,
    v1,
    c1,
    d1,
    g2,
    w2,
    v2,
    c2,
    d2,
    d3,
    solved,
    back,
    values,
    p2,
    o0,
    local_sem,
    send_sem,
    recv_sem,
):
    me, my = lax.axis_index("tm"), lax.axis_index("space")

    def peer(d):
        return lax.rem(me + d, TM)

    def slab(d):
        return lax.rem(my + (d + 8 * slabs), slabs)

    def local(src, dst, n):
        copy = pltpu.make_async_copy(src, dst, local_sem.at[n])
        copy.start()
        return copy.wait

    res_wait = local(res_in, res, 0)
    cap_wait = local(cap_in, cap, 1)
    table_wait = local(tab_in.at[me], tab, 2)

    barrier = pltpu.get_barrier_semaphore()
    greeted = 0
    for d in range(1, TM):
        pl.semaphore_signal(barrier, inc=1, device_id=(peer(d), my), device_id_type=MESH)
        greeted += 1
    for d in SHIFTS:
        if d % slabs:
            pl.semaphore_signal(barrier, inc=1, device_id=(me, slab(d)), device_id_type=MESH)
            greeted += 1
    pl.semaphore_wait(barrier, greeted)

    def remote(src, dst, out_sem, in_sem, device):
        pltpu.make_async_remote_copy(
            src_ref=src,
            dst_ref=dst,
            send_sem=send_sem.at[out_sem],
            recv_sem=recv_sem.at[in_sem],
            device_id=device,
            device_id_type=MESH,
        ).start()

    def landed(size, n):
        pltpu.make_async_copy(size, size, recv_sem.at[n]).wait()

    def sent(size, n):
        pltpu.make_async_copy(size, size, send_sem.at[n]).wait()

    def exchange(out_sem, in_sem, source, target):
        for d in (2, 1, 3):
            remote(source(peer(d)), target, out_sem, in_sem, (peer(d), my))

    res_wait()
    for l in range(2):
        exchange(
            0,
            0 + l,
            lambda j, l=l: res.at[:, layer_of(j, l)],
            series.at[pl.ds(16 * me, 16), l],
        )
    for l in range(2):
        for t in range(16):
            series[16 * me + t, l] = res[t, layer_of(me, l)]

    cap_wait()

    def spread_cap(src, dst, d):
        remote(src, dst, 7, 15, (me, slab(d)))

    spread_cap(cap.at[pl.ds(0, H0)], c0.at[pl.ds(H0 + LAYERS, H0)], -1)
    spread_cap(cap.at[pl.ds(LAYERS - H0, H0)], c0.at[pl.ds(0, H0)], 1)
    for i in range(LAYERS):
        c0[H0 + i] = cap[i]
    for i in range(LAYERS // 2):
        tile = block_sum(cap[2 * i] + cap[2 * i + 1]) * np.float32(0.125)
        c1[H1 + i] = pack(((tile, tile),) * 2)
    spread_cap(c1.at[pl.ds(H1, 4)], c1.at[pl.ds(H1 + 4, 4)], -1)
    spread_cap(c1.at[pl.ds(H1, 4)], c1.at[pl.ds(0, 4)], 1)
    for i in range(LAYERS // 4):
        tile = block_sum(c1[H1 + 2 * i] + c1[H1 + 2 * i + 1]) * np.float32(0.125)
        c2[2 * REACH + i] = pack(((tile, tile),) * 2)
    for d in SHIFTS:
        spread_cap(c2.at[pl.ds(2 * REACH, 2)], c2.at[pl.ds(2 * (REACH - d), 2)], d)

    def forward(l):
        middle = [[None] * 8 for _ in range(5)]
        for t2 in range(8):
            column = [
                (series[8 * t1 + t2, l] * np.float32(BETA ** (8 * t1 + t2)), None)
                for t1 in range(8)
            ]
            first = transform(column, -1.0)
            for k1 in range(5):
                middle[k1][t2] = twisted(first[k1], -2.0 * math.pi * k1 * t2 / LENGTH)
        for k1 in range(5):
            last = transform(middle[k1], -1.0)
            if k1 == 0:
                spec[0, 0, 0, l], spec[0, 1, 0, l] = last[0][0], last[4][0]
                chosen = [(m, 0, m) for m in (1, 2, 3)]
            elif k1 == 4:
                chosen = [(m, 0, 4 + m) for m in range(4)]
            else:
                chosen = [(m, k1, m) for m in range(8)]
            for m, j, slot in chosen:
                spec[j, 0, slot, l], spec[j, 1, slot, l] = last[m]

    for l in range(2):
        landed(series.at[pl.ds(0, 48), l], l)
        forward(l)
        for q in range(2):
            four = pl.ds(4 * q, 4)
            exchange(
                1,
                2 + 2 * l + q,
                lambda j, l=l, four=four: spec.at[j, :, four, l],
                g0.at[:, four, H0 + layer_of(me, l)],
            )
        here = H0 + layer_of(me, l)
        for c in range(2):
            for slot in range(SLOTS):
                g0[c, slot, here] = spec[me, c, slot, l]

    table_wait()
    landed(series.at[pl.ds(0, 52), 0], 15)

    def weight(index, extent):
        inside = jnp.logical_and(index >= 0, index < extent)
        return jnp.where(inside, np.float32(OMEGA), np.float32(0.0))

    six = [np.float32(6.0 * DIFFUSE / 4.0**level) for level in range(4)]

    def invert(c, first, second, third, diagonal, w):
        top, q, bottom = c * first + diagonal, c * second, c * third + diagonal
        scale = w / (top * bottom + q * q)
        return bottom * scale, q * scale, top * scale

    def invert0(slot, carry):
        first, second, third = (tab[3 * slot + k] for k in range(3))
        for i in range(N0):
            w = weight(LAYERS * my + i - H0, LAYERS * slabs)
            parts = invert(c0[i], first, second, third, six[0], w)
            for k in range(3):
                d0[slot, k, i] = parts[k]
        return carry

    lax.fori_loop(0, SLOTS, invert0, 0)
    for q in range(2):
        first, second, third = (tab[24 + 3 * q + k] for k in range(3))
        for i in range(N1):
            w = weight(4 * my + i - H1, 4 * slabs)
            parts = invert(c1[i], first, second, third, six[1], w)
            for k in range(3):
                d1[q, k, i] = parts[k]

    def diagonal(c, q, level):
        return c * tab[30 + 2 * q] + six[level], c * tab[31 + 2 * q]

    def swap(value):
        return pltpu.roll(value, 4, 0)

    def invert_packed(c, q, level, w):
        a, b = diagonal(c, q, level)
        other = swap(a)
        scale = w / (a * other + b * b)
        return other * scale, -b * scale

    for i in range(N2):
        w = weight(2 * my + i - 2 * REACH, 2 * slabs)
        for q in range(2):
            parts = invert_packed(c2[i], q, 2, w)
            d2[q, 0, i], d2[q, 1, i] = parts
    for i in range(N3):
        c = block_sum_spread(c2[2 * i + 2] + c2[2 * i + 3]) * np.float32(0.125)
        w = weight(my + i - (REACH - 1), slabs)
        for q in range(2):
            parts = invert_packed(c, q, 3, w)
            d3[q, 0, i], d3[q, 1, i] = parts

    def spread(src, dst, d, out_sem, in_sem):
        remote(src, dst, out_sem, in_sem, (me, slab(d)))

    for l in range(2):
        for q in range(2):
            four = pl.ds(4 * q, 4)
            landed(spec.at[pl.ds(0, 3), :, four, l], 2 + 2 * l + q)
            for a in range(TM):
                x = layer_of(a, l)
                here = g0.at[:, four, H0 + x]
                if x < H0:
                    spread(here, g0.at[:, four, H0 + LAYERS + x], -1, 4, 9 + q)
                if x >= LAYERS - H0:
                    spread(here, g0.at[:, four, x - (LAYERS - H0)], 1, 4, 9 + q)

    def jacobi(inverse, er, ei):
        a, b, c = inverse
        return a * er + b * ei, c * ei - b * er

    def sweep(level, below, here, above, g, inverse):
        er = g[0] - level.neighbours(below[0], here[0], above[0])
        ei = g[1] - level.neighbours(below[1], here[1], above[1])
        ur, ui = jacobi(inverse, er, ei)
        keep = np.float32(KEEP)
        return keep * here[0] + ur, keep * here[1] + ui

    def defect(level, below, here, above, g, c, shifts, six_here):
        first, second, third = shifts
        q = c * second
        er = g[0] - level.neighbours(below[0], here[0], above[0])
        ei = g[1] - level.neighbours(below[1], here[1], above[1])
        er = er - ((c * first + six_here) * here[0] - q * here[1])
        ei = ei - (q * here[0] + (c * third + six_here) * here[1])
        return er, ei

    def pre(level, layers, own, load_g, load_d, load_c, shifts, six_here, keep_v, keep_r):
        once, twice, waiting = {}, {}, None
        for i in layers:
            once[i] = jacobi(load_d(i), *load_g(i))
            if i < layers[2]:
                continue
            j = i - 1
            twice[j] = sweep(level, once[j - 1], once[j], once[j + 1], load_g(j), load_d(j))
            keep_v(j, twice[j])
            j = i - 2
            if j - own[0] in range(own[1]):
                r = defect(
                    level,
                    twice[j - 1],
                    twice[j],
                    twice[j + 1],
                    load_g(j),
                    load_c(j),
                    shifts,
                    six_here,
                )
                if (j - own[0]) % 2:
                    keep_r((j - own[0]) // 2, (waiting[0] + r[0], waiting[1] + r[1]))
                waiting = r

    def post(level, first, count, load_v, load_g, load_d, keep):
        once = {}
        start = {}
        for i in range(first - 2, first + count + 2):
            start[i] = load_v(i)
            j = i - 1
            if j < first - 1:
                continue
            once[j] = sweep(level, start[j - 1], start[j], start[j + 1], load_g(j), load_d(j))
            j = i - 2
            if j < first:
                continue
            keep(j, sweep(level, once[j - 1], once[j], once[j + 1], load_g(j), load_d(j)))

    eighth = np.float32(0.125)
    level0 = Level(0, 8, 128)
    level1 = Level(1, 4, 64)
    level2 = Level(2, 2, 32)
    level3 = Level(3, 1, 32, 2)

    def looped(start, count, together, body):
        def some(n, carry):
            for k in range(together):
                body(start + n * together + k, carry)
            return carry

        if together == count:
            some(0, 0)
        else:
            lax.fori_loop(0, count // together, some, 0)

    def views0(slot):
        return (
            lambda i: (g0[0, slot, i], g0[1, slot, i]),
            lambda i: tuple(d0[slot, k, i] for k in range(3)),
        )

    def keep0(slot, i, v):
        v0[slot, 0, i], v0[slot, 1, i] = v

    def coarsen0(slot, twice, layers, load_g):
        shifts = tuple(tab[3 * slot + k] for k in range(3))
        for i in layers:
            pair = [
                defect(
                    level0, twice[j - 1], twice[j], twice[j + 1], load_g(j), c0[j], shifts, six[0]
                )
                for j in (i, i + 1)
            ]
            for c in range(2):
                small0[slot, c, (i - H0) // 2 + OWN1] = block_sum(pair[0][c] + pair[1][c]) * eighth

    first, last = H0, H0 + LAYERS - 1

    def inside0(slot, carry):
        load_g, load_d = views0(slot)
        once, twice = {}, {}
        for i in range(first, last + 1):
            once[i] = jacobi(load_d(i), *load_g(i))
            if i - 2 >= first:
                j = i - 1
                twice[j] = sweep(level0, once[j - 1], once[j], once[j + 1], load_g(j), load_d(j))
                keep0(slot, j, twice[j])
        for n, i in enumerate((first, first + 1, last - 1, last)):
            o0[slot, 0, n], o0[slot, 1, n] = once[i]
        coarsen0(slot, twice, range(first + 2, last - 2, 2), load_g)
        return carry

    def outside0(slot, carry):
        load_g, load_d = views0(slot)
        for edge, step, stored in ((first, -1, (0, 1)), (last, 1, (3, 2))):
            once = {
                edge: (o0[slot, 0, stored[0]], o0[slot, 1, stored[0]]),
                edge - step: (o0[slot, 0, stored[1]], o0[slot, 1, stored[1]]),
            }
            twice = {
                i: (v0[slot, 0, i], v0[slot, 1, i]) for i in (edge - step, edge - 2 * step)
            }
            for n in range(1, H0 + 1):
                i = edge + n * step
                once[i] = jacobi(load_d(i), *load_g(i))
                j = i - step
                twice[j] = sweep(level0, once[j - 1], once[j], once[j + 1], load_g(j), load_d(j))
                if n <= 3:
                    keep0(slot, j, twice[j])
            pairs = [min(edge - step, edge) + 2 * n * step for n in range(1 + OWN1)]
            coarsen0(slot, twice, pairs, load_g)
        return carry

    for q in range(2):
        looped(4 * q, 4, 4, inside0)

    def views1(q):
        return (
            lambda i: (g1[q, 0, i], g1[q, 1, i]),
            lambda i: tuple(d1[q, k, i] for k in range(3)),
        )

    for q in range(2):
        landed(g0.at[:, pl.ds(4 * q, 4), pl.ds(0, 2 * H0)], 9 + q)
        looped(4 * q, 4, 2, outside0)
        for c in range(2):
            for i in range(4 + 2 * OWN1):
                tiles = [[small0[4 * q + 2 * sb + lb, c, i] for lb in range(2)] for sb in range(2)]
                g1[q, c, H1 - OWN1 + i] = pack(tiles)
        far = H1 - OWN1
        spread(g1.at[q, :, pl.ds(H1, far)], g1.at[q, :, pl.ds(0, far)], 1, 5, 11 + q)
        spread(
            g1.at[q, :, pl.ds(H1 + 4 - far, far)],
            g1.at[q, :, pl.ds(N1 - far, far)],
            -1,
            5,
            11 + q,
        )

        coarse = {}

        def keep_v(i, v, q=q):
            v1[q, 0, i], v1[q, 1, i] = v

        def keep_r(i, r, coarse=coarse):
            for c in range(2):
                coarse[c, i] = block_sum(r[c]) * eighth

        load_g, load_d = views1(q)
        pre(
            level1,
            range(H1 - OWN1, H1 + 4 + OWN1),
            (H1, 4),
            load_g,
            load_d,
            lambda i: c1[i],
            tuple(tab[24 + 3 * q + k] for k in range(3)),
            six[1],
            keep_v,
            keep_r,
        )
        p2[q, REACH] = pack([[coarse[c, 0], coarse[c, 1]] for c in range(2)])
        for d in SHIFTS:
            spread(p2.at[q, REACH], p2.at[q, REACH - d], d, 6, 13 + q)

    for q in range(2):
        landed(g1.at[q, :, pl.ds(0, 2 * (H1 - OWN1))], 11 + q)
        load_g, load_d = views1(q)
        for low in (0, N1 - 4):
            once = {i: jacobi(load_d(i), *load_g(i)) for i in range(low, low + 4)}
            for i in (low + 1, low + 2):
                v = sweep(level1, once[i - 1], once[i], once[i + 1], load_g(i), load_d(i))
                v1[q, 0, i], v1[q, 1, i] = v

    def relax(d, q, i, e):
        return d[q, 0, i] * e + d[q, 1, i] * swap(e)

    def sweep_packed(level, below, here, above, g, d, q, i):
        return np.float32(KEEP) * here + relax(d, q, i, g - level.neighbours(below, here, above))

    def coarse_levels(q):
        for i in range(N2 // 2):
            g2[q, 2 * i], g2[q, 2 * i + 1] = p2[q, i], pltpu.roll(p2[q, i], 64, 1)
        for i in range(N2):
            w2[i] = relax(d2, q, i, g2[q, i])
        for i in range(1, N2 - 1):
            v2[i] = sweep_packed(level2, w2[i - 1], w2[i], w2[i + 1], g2[q, i], d2, q, i)
        right = []
        for m in range(N3):
            pair = []
            for i in (2 * m + 2, 2 * m + 3):
                here = v2[i]
                a, b = diagonal(c2[i], q, 2)
                pair.append(
                    g2[q, i]
                    - level2.neighbours(v2[i - 1], here, v2[i + 1])
                    - (a * here + b * swap(here))
                )
            right.append(block_sum_spread(pair[0] + pair[1]) * eighth)
        current = {m: relax(d3, q, m, right[m]) for m in range(N3)}
        for s in range(1, 6):
            current = {
                m: sweep_packed(
                    level3, current[m - 1], current[m], current[m + 1], right[m], d3, q, m
                )
                for m in range(s, N3 - s)
            }
        low = 2 * 5 + 2
        stage = {i: v2[i] + current[(i - 2) // 2] for i in range(low, low + 10)}
        for s in range(1, 3):
            stage = {
                i: sweep_packed(level2, stage[i - 1], stage[i], stage[i + 1], g2[q, i], d2, q, i)
                for i in range(low + s, low + 10 - s)
            }
        return stage

    def up1(q, stage):
        correction = {}

        def load_v(i):
            m = 2 * REACH + (i - H1) // 2
            if m not in correction:
                correction[m] = [unpack(stage[m], c, 0) for c in range(2)]
            return tuple(v1[q, c, i] + correction[m][c] for c in range(2))

        def keep(i, v):
            v1[q, 0, i], v1[q, 1, i] = v

        post(
            level1,
            H1 - 1,
            6,
            load_v,
            *views1(q),
            keep,
        )

    def up0(q, k, carry):
        slot, sb, lb = 4 * q + k, k >> 1, k & 1
        correction = {}

        def load_v(i):
            m = H1 + (i - H0) // 2
            if m not in correction:
                correction[m] = [unpack(v1[q, c, m], sb, lb) for c in range(2)]
            return tuple(v0[slot, c, i] + correction[m][c] for c in range(2))

        def keep(i, v):
            solved[0, slot, i - H0], solved[1, slot, i - H0] = v

        post(
            level0,
            H0,
            LAYERS,
            load_v,
            lambda i: (g0[0, slot, i], g0[1, slot, i]),
            lambda i: tuple(d0[slot, k, i] for k in range(3)),
            keep,
        )
        return carry

    for q in range(2):
        landed(p2.at[q, pl.ds(0, 2 * REACH)], 13 + q)
        stage = coarse_levels(q)
        up1(q, stage)
        for k, size in ((0, 2), (2, 2)) if q == 0 else ((0, 4),):
            looped(k, size, 2, lambda k, carry, q=q: up0(q, k, carry))
            some = pl.ds(4 * q + k, size)
            for l in range(2):
                exchange(
                    2,
                    6 + l,
                    lambda j, l=l, some=some: solved.at[:, some, layer_of(j, l)],
                    back.at[me, :, some, l],
                )
        for l in range(2):
            for c in range(2):
                for slot in range(4 * q, 4 * q + 4):
                    back[me, c, slot, l] = solved[c, slot, layer_of(me, l)]

    def inverse(l):
        def field(j, slot, factor=2.0):
            return tuple(back[j, c, slot, l] * np.float32(factor) for c in range(2))

        nothing = (None, None)
        packed = field(0, 0, 1.0)
        line = [(packed[0], None)] + [field(0, m) for m in (1, 2, 3)] + [(packed[1], None)]
        line = transform(line + [nothing] * 3, 1.0)
        middle = [[(line[t2][0], None) for t2 in range(8)]]
        for k1 in (1, 2, 3):
            line = transform([field(k1, m) for m in range(8)], 1.0)
            middle.append(
                [twisted(line[t2], 2.0 * math.pi * k1 * t2 / LENGTH) for t2 in range(8)]
            )
        line = transform([field(0, 4 + m) for m in range(4)] + [nothing] * 4, 1.0)
        turned = [twisted(line[t2], 2.0 * math.pi * 4 * t2 / LENGTH) for t2 in range(8)]
        middle.append([(turned[t2][0], None) for t2 in range(8)])
        for t2 in range(8):
            column = transform([middle[k1][t2] for k1 in range(5)] + [nothing] * 3, 1.0)
            for t1 in range(8):
                t = 8 * t1 + t2
                values[l, t] = column[t1][0] * np.float32(BETA ** (-t) / LENGTH)

    for l in range(2):
        landed(back.at[pl.ds(0, 3), :, :, l], 6 + l)
        inverse(l)
        mine = out.at[:, layer_of(me, l)]
        exchange(3, 8, lambda j, l=l: values.at[l, pl.ds(16 * j, 16)], mine)
        for t in range(16):
            out[t, layer_of(me, l)] = values[l, 16 * me + t]
    sent(series.at[pl.ds(0, 48)], 0)
    sent(spec.at[pl.ds(0, 3)], 1)
    sent(back.at[pl.ds(0, 3)], 2)
    sent(g0.at[:, :, pl.ds(0, 2 * H0)], 4)
    sent(g1.at[:, :, pl.ds(0, 2 * (H1 - OWN1))], 5)
    sent(p2.at[:, pl.ds(0, 2 * REACH)], 6)
    sent(series.at[pl.ds(0, 52), 0], 7)
    sent(values.at[:, pl.ds(0, 48)], 3)
    landed(values.at[:, pl.ds(0, 48)], 8)


def write_out(src, dst, sem):
    copy = pltpu.make_async_copy(src, dst, sem.at[0])
    copy.start()
    copy.wait()


def solution(mesh):
    slabs = mesh.shape["space"]
    table = shift_tables()

    def tiles(*lead):
        return pltpu.VMEM(lead + (8, 128), F32)

    def on_device(residual, capacity):
        any_space = pl.BlockSpec(memory_space=pl.ANY)
        dma = pltpu.SemaphoreType.DMA
        result = pl.pallas_call(
            lambda *refs: kernel(slabs, *refs),
            out_shape=jax.ShapeDtypeStruct(residual.shape, F32),
            in_specs=[any_space] * 3,
            out_specs=pl.BlockSpec(memory_space=pltpu.VMEM),
            scratch_shapes=[
                tiles(16, LAYERS),
                tiles(LAYERS),
                tiles(34),
                tiles(LENGTH, 2),
                tiles(TM, 2, SLOTS, 2),
                tiles(2, SLOTS, N0),
                tiles(SLOTS, 2, N0),
                tiles(N0),
                tiles(SLOTS, 3, N0),
                tiles(SLOTS, 2, 4 + 2 * OWN1),
                tiles(2, 2, N1),
                tiles(2, 2, N1),
                tiles(N1),
                tiles(2, 3, N1),
                tiles(2, N2),
                tiles(N2),
                tiles(N2),
                tiles(N2),
                tiles(2, 2, N2),
                tiles(2, 2, N3),
                tiles(2, SLOTS, LAYERS),
                tiles(TM, 2, SLOTS, 2),
                tiles(2, LENGTH),
                tiles(2, 1 + 2 * REACH),
                tiles(SLOTS, 2, 4),
                dma((3,)),
                dma((8,)),
                dma((16,)),
            ],
            compiler_params=pltpu.CompilerParams(collective_id=0, has_side_effects=True, vmem_limit_bytes=24 << 20),
            name="paradiag",
        )(*(pltpu.with_memory_space_constraint(v, pltpu.HBM) for v in (residual, capacity, jnp.asarray(table))))
        return pl.pallas_call(
            write_out,
            out_shape=jax.ShapeDtypeStruct(residual.shape, F32),
            in_specs=[pl.BlockSpec(memory_space=pltpu.VMEM)],
            out_specs=any_space,
            scratch_shapes=[dma((1,))],
            compiler_params=pltpu.CompilerParams(vmem_limit_bytes=1 << 20),
            name="write_out",
        )(result)

    return jax.shard_map(
        on_device,
        mesh=mesh,
        in_specs=(P("tm", "space", None, None), P("space", None, None)),
        out_specs=P("tm", "space", None, None),
        check_vma=False,
    )
```
